256 devices in a mesh: wav: 32 (over y, x, core), lev: 8 (over z).
Axes of the slice: x: 4, y: 4, z: 8, core: 2. Of those that a mesh axis runs over, the one named last changes fastest.
Arguments:
- spectral: bfloat16 [224, 401, 1024], P('wav', None, 'lev'), may hold values from -0.1796875 to 0.1796875
- legendre: bfloat16 [224, 401, 256], P('wav', None, 'lev'), may hold values from -0.4375 to 0.4375
- wave_pair: int32 [224], replicated, may hold values from -1 to 199, as said below
- lat_slot: int32 [256], replicated, may hold values from 0 to 799, as said below
Outputs:
- gridded: bfloat16 [256, 512, 1616], P('wav', 'lev')
The draws below stay inside these ranges and needn't reach their ends.
Inputs may be any that keep to these rules, and one draw needn't show every extreme that they name: `wave_pair`: each pair number 0 to 199 appears exactly once; all other entries are -1. `lat_slot`: the entries are distinct latitudes.
All inputs are finite; a program needn't handle non-finite values.
Results may differ from the reference program's by a relative error of at most 0.0055.
Values may be sent and summed in bfloat16 or wider, within the bound.
A program may use at most 64 MiB of HBM per device.

```python
import math
import jax
import jax.numpy as jnp
from jax import lax

WAVES = 400
NLAT = 800
PAIRS = 200
FOLD = 401
WSLOTS = 224
NROWS = 256
LAYERS = 512


def draw_wave_pair(key, part):
    order = jax.random.permutation(jax.random.fold_in(key, 11), WSLOTS)
    return jnp.where(order < PAIRS, order, -1).astype(jnp.int32)


def draw_lat_slot(key, part):
    order = jax.random.permutation(jax.random.fold_in(key, 13), NLAT)
    return order[:NROWS].astype(jnp.int32)


def levels(own_key, extent, shards, least, high):
    gain = 1.0
    for dim, parts in shards:
        heights = jax.random.uniform(jax.random.fold_in(jax.random.fold_in(own_key, 6), dim), (parts,), jnp.float32, least / len(shards), high / len(shards))
        gain = gain * jnp.repeat(jnp.exp(heights), extent[dim] // parts).reshape((-1,) + (1,) * (len(extent) - 1 - dim))
    return gain


def noise(stream_key, shape, scale, bound, pieces=(), kind=jnp.bfloat16):
    entries = scale * jax.random.normal(stream_key, shape, jnp.float32)
    if pieces:
        entries = entries * levels(stream_key, shape, pieces, -0.22, 0.18)
    return jnp.clip(entries, -bound, bound).astype(kind)


def setup_inputs(seed: int = 0) -> dict:
    seeds = jax.random.split(jax.random.key(seed), 5)
    spectral = noise(seeds[0], (WSLOTS, FOLD, 2 * LAYERS), 0.03, 0.1796875, ((0, 32), (2, 8)))
    legendre = noise(seeds[1], (WSLOTS, FOLD, NROWS), (WAVES // 2) ** -0.5, 0.4375, ((0, 32), (2, 8)))
    wave_pair = draw_wave_pair(jax.random.fold_in(seeds[4], 71), 0)
    lat_slot = draw_lat_slot(jax.random.fold_in(seeds[4], 71), 0)
    return {"spectral": spectral, "legendre": legendre, "wave_pair": wave_pair, "lat_slot": lat_slot}


def fold_masks(pair_ids, fold_count, wave_count):
    fold_rows = jnp.arange(fold_count, dtype=jnp.int32)
    filled = pair_ids >= 0
    border = wave_count - pair_ids
    lower = filled[:, None] & (fold_rows[None, :] < border[:, None])
    upper = filled[:, None] & (fold_rows[None, :] >= border[:, None])
    return jnp.stack([lower, upper], axis=1)


def trig_parts(wave_numbers, steps, counts_b):
    residue = (wave_numbers[None, None] * steps[None, :, None, None]) % counts_b
    angles = residue.astype(jnp.float32) * (2.0 * math.pi) / counts_b.astype(jnp.float32)
    return jnp.cos(angles), jnp.sin(angles)


def synthesis_table(pair_ids, row_lats, lat_count, lon_width, wave_count):
    filled = pair_ids >= 0
    wave_numbers = jnp.stack([pair_ids, wave_count - 1 - pair_ids], axis=1)
    lon_count = 20 + 4 * jnp.minimum(row_lats, lat_count - 1 - row_lats)
    highest = jnp.minimum(wave_count - 1, (lon_count - 1) // 2)
    counts_b = lon_count[:, None, None, None]
    coarse_count = (lon_width + 63) // 64
    coarse_steps = jnp.arange(coarse_count, dtype=jnp.int32) * 64
    fine_steps = jnp.arange(64, dtype=jnp.int32)
    cos_coarse, sin_coarse = trig_parts(wave_numbers, coarse_steps, counts_b)
    cos_fine, sin_fine = trig_parts(wave_numbers, fine_steps, counts_b)
    cos_all = cos_coarse[:, :, None] * cos_fine[:, None] - sin_coarse[:, :, None] * sin_fine[:, None]
    sin_all = sin_coarse[:, :, None] * cos_fine[:, None] + cos_coarse[:, :, None] * sin_fine[:, None]
    row_total = row_lats.shape[0]
    cos_all = cos_all.reshape(row_total, coarse_count * 64, wave_numbers.shape[0], 2)[:, :lon_width]
    sin_all = sin_all.reshape(row_total, coarse_count * 64, wave_numbers.shape[0], 2)[:, :lon_width]
    columns = jnp.arange(lon_width, dtype=jnp.int32)
    valid = filled[None, None, :, None] & (wave_numbers[None, None] <= highest[:, None, None, None]) & (columns[None, :, None, None] < counts_b)
    factor = jnp.where(wave_numbers == 0, 1.0, 2.0).astype(jnp.float32)[None, None]
    real_part = jnp.where(valid, factor * cos_all, 0.0)
    imag_part = jnp.where(valid, -factor * sin_all, 0.0)
    return jnp.stack([real_part, imag_part], axis=-1).astype(jnp.bfloat16)


def reference(spectral, legendre, wave_pair, lat_slot):
    fold_count = spectral.shape[1]
    wave_count = fold_count - 1
    lat_count = NLAT
    lon_width = 2 * lat_count + 16
    layer_count = spectral.shape[2] // 2
    row_total = lat_slot.shape[0]
    half_masks = fold_masks(wave_pair, fold_count, wave_count)
    paired = spectral.reshape(spectral.shape[0], fold_count, layer_count, 2)

    def per_slot(args):
        coefficients, weights, masks_one = args
        masked = jnp.where(masks_one[:, :, None, None], coefficients.astype(jnp.float32)[None], 0.0)
        summed = jnp.einsum("htlc,ta->ahcl", masked, weights.astype(jnp.float32))
        return summed.astype(jnp.bfloat16)

    fourier = lax.map(per_slot, (paired, legendre, half_masks))

    def per_row(args):
        latitude, position = args
        basis = synthesis_table(wave_pair, latitude[None], lat_count, lon_width, wave_count)[0]
        picked = jnp.take(fourier, position, axis=1)
        flat_basis = basis.reshape(lon_width, -1).astype(jnp.float32)
        flat_values = picked.reshape(-1, layer_count).astype(jnp.float32)
        result = jnp.dot(flat_basis, flat_values, preferred_element_type=jnp.float32)
        return result.T.astype(jnp.bfloat16)

    positions = jnp.arange(row_total, dtype=jnp.int32)
    return lax.map(per_row, (lat_slot, positions))
```

```python
import functools
import math

import jax
import jax.numpy as jnp
import numpy as np
from jax import lax
from jax.experimental import pallas as pl
from jax.experimental.pallas import tpu as pltpu
from jax.sharding import PartitionSpec as P

NLAT = 800
WIDTH = 256
MESH = pl.DeviceIdType.MESH


def poly_in_square(fn, degree):
    nodes = np.cos(np.pi * (np.arange(200) + 0.5) / 200)
    top = 0.52**2
    z = (nodes + 1) * 0.5 * top
    fit = np.polynomial.chebyshev.Chebyshev.fit(z, fn(np.sqrt(z)), degree, domain=[0, top])
    return [float(c) for c in fit.convert(kind=np.polynomial.Polynomial).coef]


SIN_COEF = poly_in_square(lambda x: np.sin(np.pi * x) / x, 5)
COS_COEF = poly_in_square(lambda x: np.cos(np.pi * x), 5)


def horner(coef, z):
    acc = jnp.full_like(z, coef[-1])
    for c in coef[-2::-1]:
        acc = acc * z + c
    return acc


def half_angle(steps, count, inverse):
    turns = jnp.floor(steps * inverse + 0.5)
    x = (steps - turns * count) * inverse
    z = x * x
    return x * horner(SIN_COEF, z), horner(COS_COEF, z)


def exchange_kernel(
    slots, fold, tiles, batches, pair_ref, leg_ref, spec_ref, out_ref, held, rhs, ready, send_sem, recv_sem, out_send, out_recv, own_sem
):
    wav_count = lax.axis_size("wav")
    lev_count = lax.axis_size("lev")
    w = lax.axis_index("wav")
    z = lax.axis_index("lev")
    right = lax.rem(z + 1, lev_count)
    left = lax.rem(z + lev_count - 1, lev_count)
    block = leg_ref.shape[1]
    full = (fold // 128) * 128
    rest = fold - full
    per_slot = full // 128
    chunk = held.shape[2]

    barrier = pltpu.get_barrier_semaphore()
    for peer in (left, right):
        pl.semaphore_signal(barrier, inc=1, device_id={"lev": peer}, device_id_type=MESH)

    def greet(k, _):
        peer = lax.rem(w + k, wav_count)
        pl.semaphore_signal(barrier, inc=1, device_id={"wav": peer}, device_id_type=MESH)
        return 0

    lax.fori_loop(1, wav_count, greet, 0)

    tail = jnp.zeros((block, 128), jnp.float32)
    for s in range(slots):
        rows = lax.broadcasted_iota(jnp.int32, (rest, 128), 0)
        cols = lax.broadcasted_iota(jnp.int32, (rest, 128), 1)
        place = (cols == rows + rest * s).astype(jnp.bfloat16)
        tail += jnp.dot(leg_ref[s, :, full:fold], place, preferred_element_type=jnp.float32)
    held[z, 0, 0] = tail.astype(jnp.bfloat16)
    for s in range(slots):
        for k in range(per_slot):
            i = 1 + s * per_slot + k
            held[z, i // chunk, i % chunk] = leg_ref[s, :, k * 128 : (k + 1) * 128]

    pl.semaphore_wait(barrier, 2 + wav_count - 1)

    half = lev_count // 2

    def goes(side, d, c):
        return d < half - 1 or c % 2 == side

    def hop(side, d, c):
        owner = lax.rem(z + (lev_count - d if side == 0 else d), lev_count)
        return pltpu.make_async_remote_copy(
            src_ref=held.at[owner, c],
            dst_ref=held.at[owner, c],
            send_sem=send_sem.at[side, d, c],
            recv_sem=recv_sem.at[side, d, c],
            device_id={"lev": right if side == 0 else left},
            device_id_type=MESH,
        )

    def arrived(side, d, c):
        owner = lax.rem(z + (lev_count - d - 1 if side == 0 else d + 1), lev_count)
        pltpu.make_async_remote_copy(
            src_ref=held.at[owner, c],
            dst_ref=held.at[owner, c],
            send_sem=send_sem.at[side, d, c],
            recv_sem=recv_sem.at[side, d, c],
            device_id={"lev": right if side == 0 else left},
            device_id_type=MESH,
        ).wait_recv()

    def own(batch):
        for c in batch:
            for side in (0, 1):
                hop(side, 0, c).start()

    def forward(batch, d):
        for c in batch:
            for side in (0, 1):
                arrived(side, d - 1, c)
                if goes(side, d, c):
                    hop(side, d, c).start()

    landed = set()

    def last(c):
        if c not in landed:
            landed.add(c)
            arrived(c % 2, half - 1, c)

    def one_slot(s):
        parts = [0] + [1 + s * per_slot + k for k in range(per_slot)]
        for i in parts:
            last(i // chunk)
        total = None
        for a in range(0, len(parts), 2):
            pieces = [
                held[:, i // chunk, i % chunk].reshape(lev_count * block, 128) for i in parts[a : a + 2]
            ]
            lhs = jnp.concatenate(pieces, axis=1)
            term = jnp.dot(lhs, rhs[s, a * 128 : (a + 2) * 128], preferred_element_type=jnp.float32)
            total = term if total is None else total + term
        groups = total.reshape(wav_count, total.shape[0] // wav_count, 256)
        both = jnp.concatenate([groups[:, :, :128], groups[:, :, 128:]], axis=1)
        ready[s] = both.astype(jnp.bfloat16)

        def send(k, _):
            peer = lax.rem(w + k, wav_count)
            pltpu.make_async_remote_copy(
                src_ref=ready.at[s, peer],
                dst_ref=out_ref.at[w, s],
                send_sem=out_send,
                recv_sem=out_recv.at[w],
                device_id={"wav": peer},
                device_id_type=MESH,
            ).start()
            return 0

        lax.fori_loop(1, wav_count, send, 0)
        pltpu.make_async_copy(ready.at[s, w], out_ref.at[w, s], own_sem).start()

    own(batches[0])

    for s in range(slots):
        border = (fold - 1) - pair_ref[w * slots + s]
        rows = lax.broadcasted_iota(jnp.int32, (128, rest), 0)
        cols = lax.broadcasted_iota(jnp.int32, (128, rest), 1)
        place = (rows == cols + rest * s).astype(jnp.bfloat16)
        row = lax.broadcasted_iota(jnp.int32, (128, 128), 0)
        ending = jnp.dot(place, spec_ref[s, full:fold, :], preferred_element_type=jnp.float32)
        below = row - rest * s + full < border
        rhs[s, 0:128, 0:128] = jnp.where(below, ending, 0.0).astype(jnp.bfloat16)
        rhs[s, 0:128, 128:256] = jnp.where(below, 0.0, ending).astype(jnp.bfloat16)
        for k in range(per_slot):
            piece = spec_ref[s, k * 128 : (k + 1) * 128, :].astype(jnp.float32)
            below = row + k * 128 < border
            at = (k + 1) * 128
            rhs[s, at : at + 128, 0:128] = jnp.where(below, piece, 0.0).astype(jnp.bfloat16)
            rhs[s, at : at + 128, 128:256] = jnp.where(below, 0.0, piece).astype(jnp.bfloat16)

    todo = list(range(slots))
    for b, batch in enumerate(batches):
        if b:
            own(batch)
        seen = set(c for earlier in batches[:b] for c in earlier)
        for d in range(1, half):
            while b and todo:
                s = todo[0]
                if all((1 + s * per_slot + k) // chunk in seen for k in range(per_slot)):
                    one_slot(todo.pop(0))
                    break
                break
            forward(batch, d)
    for s in todo:
        one_slot(s)
    for c in range(held.shape[1]):
        last(c)

    for side in (0, 1):
        for d in range(half):
            for c in range(held.shape[1]):
                if goes(side, d, c):
                    hop(side, d, c).wait_send()

    def arrival(k, _):
        peer = lax.rem(w + k, wav_count)
        pltpu.make_async_copy(out_ref.at[peer], out_ref.at[peer], out_recv.at[peer]).wait()
        return 0

    lax.fori_loop(1, wav_count, arrival, 0)
    pltpu.make_async_copy(ready.at[:, 1:], ready.at[:, 1:], out_send).wait()
    pltpu.make_async_copy(out_ref.at[w], out_ref.at[w], own_sem).wait()


def exchange(spectral, legendre, wave_pair):
    slots, fold, _ = spectral.shape
    wav_count = lax.axis_size("wav")
    lev_count = lax.axis_size("lev")
    block = legendre.shape[2]
    rows = block * lev_count // wav_count
    turned = jnp.swapaxes(legendre, 1, 2)
    tiles = 1 + slots * (fold // 128)
    chunk = 2
    chunks = tiles // chunk
    batches = [list(range(6)), list(range(6, chunks))]
    half = lev_count // 2
    return pl.pallas_call(
        functools.partial(exchange_kernel, slots, fold, tiles, batches),
        out_shape=jax.ShapeDtypeStruct((wav_count, slots, 2 * rows, 128), jnp.bfloat16),
        in_specs=[
            pl.BlockSpec(memory_space=pltpu.SMEM),
            pl.BlockSpec(memory_space=pltpu.VMEM),
            pl.BlockSpec(memory_space=pltpu.VMEM),
        ],
        out_specs=pl.BlockSpec(memory_space=pl.ANY),
        scratch_shapes=[
            pltpu.VMEM((lev_count, chunks, chunk, block, 128), jnp.bfloat16),
            pltpu.VMEM((slots, 512, 256), jnp.bfloat16),
            pltpu.VMEM((slots, wav_count, 2 * rows, 128), jnp.bfloat16),
            pltpu.SemaphoreType.DMA((2, half, chunks)),
            pltpu.SemaphoreType.DMA((2, half, chunks)),
            pltpu.SemaphoreType.DMA,
            pltpu.SemaphoreType.DMA((wav_count,)),
            pltpu.SemaphoreType.DMA,
        ],
        compiler_params=pltpu.CompilerParams(collective_id=0, has_side_effects=True),
        name="exchange",
    )(wave_pair, turned, spectral)


def synthesis_kernel(waves, rows, pair_ref, lat_ref, in_ref, out_ref, flat, column, table, turned, half_turn):
    r = pl.program_id(0)
    slots = pair_ref.shape[1]
    layers = out_ref.shape[1]
    width = out_ref.shape[2]
    blocks = (width + WIDTH - 1) // WIDTH

    @pl.when(r == 0)
    def _():
        flat[...] = in_ref[...].astype(jnp.float32)
        pairs = pair_ref[...].astype(jnp.float32)
        column[...] = jnp.transpose(jnp.broadcast_to(pairs, (128, slots)))
        table[...] = jnp.zeros_like(table)
        turned[...] = jnp.zeros_like(turned)

    a = lat_ref[lax.axis_index("wav") * rows + r]
    lon = 20 + 4 * jnp.minimum(a, NLAT - 1 - a)
    highest = jnp.minimum(waves - 1, lax.shift_right_arithmetic(lon - 1, 1)).astype(jnp.float32)
    count = lon.astype(jnp.float32)
    count_col = jnp.full((slots, 128), count, jnp.float32)
    inverse_col = 1.0 / count_col
    lane = lax.broadcasted_iota(jnp.int32, (slots, 128), 1).astype(jnp.float32)

    for h in range(2):
        pair = column[...]
        m = pair if h == 0 else (waves - 1.0) - pair
        weight = jnp.where(m == 0.0, 1.0, 2.0)
        weight = jnp.where((pair >= 0.0) & (m <= highest), weight, 0.0)
        minus = -2.0 * weight
        for c in range(WIDTH // 128):
            sin_half, cos_half = half_angle(m * (lane + 128.0 * c), count_col, inverse_col)
            scaled = sin_half * minus
            at = pl.ds(h * 256, slots)
            table[at, c * 128 : (c + 1) * 128] = (weight + scaled * sin_half).astype(jnp.bfloat16)
            at = pl.ds(512 + h * 256, slots)
            table[at, c * 128 : (c + 1) * 128] = (scaled * cos_half).astype(jnp.bfloat16)

    target = lax.broadcasted_iota(jnp.int32, (128, 128), 0)
    source = lax.broadcasted_iota(jnp.int32, (128, 128), 1)
    part = (target >= layers).astype(jnp.int32)
    place = (source == 2 * (target - part * layers) + part).astype(jnp.bfloat16)
    count_row = jnp.full((8, slots), count, jnp.float32)
    inverse_row = 1.0 / count_row
    shift = lax.broadcasted_iota(jnp.int32, (8, slots), 0).astype(jnp.float32) * WIDTH
    for h in range(2):
        values = flat[pl.ds(h * rows + r, slots, stride=2 * rows), :].astype(jnp.bfloat16)
        split = lax.dot_general(
            place, values, (((1,), (1,)), ((), ())), preferred_element_type=jnp.float32
        )
        real, imag = split[:layers], split[layers:]
        pairs = jnp.broadcast_to(pair_ref[...].astype(jnp.float32), (8, slots))
        m = pairs if h == 0 else (waves - 1.0) - pairs
        sin_half, cos_half = half_angle(m * shift, count_row, inverse_row)
        sines = 2.0 * sin_half * cos_half
        cosines = 1.0 - 2.0 * sin_half * sin_half
        for b in range(blocks):
            at = pl.ds(b * layers, layers)
            if b == 0:
                turned_real, turned_imag = real, imag
            else:
                cos_b, sin_b = cosines[b : b + 1], sines[b : b + 1]
                turned_real = real * cos_b - imag * sin_b
                turned_imag = real * sin_b + imag * cos_b
            turned[at, h * 256 : h * 256 + slots] = turned_real.astype(jnp.bfloat16)
            turned[at, 512 + h * 256 : 512 + h * 256 + slots] = turned_imag.astype(jnp.bfloat16)

    result = jnp.dot(turned[...], table[...], preferred_element_type=jnp.float32)
    for b in range(blocks):
        size = min(WIDTH, width - b * WIDTH)
        col = lax.broadcasted_iota(jnp.int32, (layers, size), 1) + b * WIDTH
        piece = result[b * layers : (b + 1) * layers, :size]
        out_ref[0, :, b * WIDTH : b * WIDTH + size] = jnp.where(col < lon, piece, 0.0).astype(jnp.bfloat16)


def synthesis(received, wave_pair, lat_slot, waves):
    wav_count, slots, both, _ = received.shape
    rows = both // 2
    total = wav_count * slots
    layers = 64
    width = 2 * NLAT + 16
    blocks = (width + WIDTH - 1) // WIDTH
    flat = received.reshape(total * both, 128)
    return pl.pallas_call(
        functools.partial(synthesis_kernel, waves, rows),
        grid=(rows,),
        out_shape=jax.ShapeDtypeStruct((rows, layers, width), jnp.bfloat16),
        in_specs=[
            pl.BlockSpec((1, total), lambda r: (0, 0)),
            pl.BlockSpec(memory_space=pltpu.SMEM),
            pl.BlockSpec((total * both, 128), lambda r: (0, 0)),
        ],
        out_specs=pl.BlockSpec((1, layers, width), lambda r: (r, 0, 0)),
        scratch_shapes=[
            pltpu.VMEM((total * both, 128), jnp.float32),
            pltpu.VMEM((total, 128), jnp.float32),
            pltpu.VMEM((1024, WIDTH), jnp.bfloat16),
            pltpu.VMEM((blocks * layers, 1024), jnp.bfloat16),
            pltpu.VMEM((8, 128), jnp.float32),
        ],
        compiler_params=pltpu.CompilerParams(dimension_semantics=("arbitrary",)),
        name="synthesis",
    )(wave_pair.reshape(1, total), lat_slot, flat)


def on_device(spectral, legendre, wave_pair, lat_slot):
    received = exchange(spectral, legendre, wave_pair)
    return synthesis(received, wave_pair, lat_slot, spectral.shape[1] - 1)


def solution(mesh):
    return jax.shard_map(
        on_device,
        mesh=mesh,
        in_specs=(P("wav", None, "lev"), P("wav", None, "lev"), P(), P()),
        out_specs=P("wav", "lev", None),
        check_vma=False,
    )
```

```python
import functools

import jax
import jax.numpy as jnp
import numpy as np
from jax import lax
from jax.experimental import pallas as pl
from jax.experimental.pallas import tpu as pltpu
from jax.sharding import PartitionSpec as P

NLAT = 800
WIDTH = 256
MESH = pl.DeviceIdType.MESH


def poly_in_square(fn, degree):
    nodes = np.cos(np.pi * (np.arange(200) + 0.5) / 200)
    top = 0.52**2
    z = (nodes + 1) * 0.5 * top
    fit = np.polynomial.chebyshev.Chebyshev.fit(z, fn(np.sqrt(z)), degree, domain=[0, top])
    return [float(c) for c in fit.convert(kind=np.polynomial.Polynomial).coef]


SIN_COEF = poly_in_square(lambda x: np.sin(np.pi * x) / x, 5)
COS_COEF = poly_in_square(lambda x: np.cos(np.pi * x), 5)


def horner(coef, z):
    acc = jnp.full_like(z, coef[-1])
    for c in coef[-2::-1]:
        acc = acc * z + c
    return acc


def half_angle(steps, count, inverse):
    turns = jnp.floor(steps * inverse + 0.5)
    x = (steps - turns * count) * inverse
    z = x * x
    return x * horner(SIN_COEF, z), horner(COS_COEF, z)


def exchange_kernel(
    waves,
    slots,
    fold,
    order,
    pair_hbm,
    pairs_hbm,
    lat_hbm,
    leg_hbm,
    spec_hbm,
    out_ref,
    table_hbm,
    pair_ref,
    pairs_ref,
    lat_ref,
    leg_ref,
    spec_ref,
    held,
    rhs,
    ready,
    table,
    column,
    load_sem,
    send_sem,
    recv_sem,
    out_send,
    out_recv,
    own_sem,
    table_sem,
):
    wav_count = lax.axis_size("wav")
    lev_count = lax.axis_size("lev")
    w = lax.axis_index("wav")
    z = lax.axis_index("lev")
    right = lax.rem(z + 1, lev_count)
    left = lax.rem(z + lev_count - 1, lev_count)
    block = leg_ref.shape[1]
    full = (fold // 128) * 128
    rest = fold - full
    per_slot = full // 128
    chunks = held.shape[1]
    chunk = held.shape[2]
    rows = table.shape[0]
    total_slots = column.shape[0]

    sources = ((leg_hbm, leg_ref), (pair_hbm, pair_ref), (pairs_hbm, pairs_ref), (lat_hbm, lat_ref), (spec_hbm, spec_ref))
    loads = [pltpu.make_async_copy(src, dst, load_sem.at[i]) for i, (src, dst) in enumerate(sources)]
    for load in loads:
        load.start()

    barrier = pltpu.get_barrier_semaphore()
    for peer in (left, right):
        pl.semaphore_signal(barrier, inc=1, device_id={"lev": peer}, device_id_type=MESH)

    def greet(k, _):
        peer = lax.rem(w + k, wav_count)
        pl.semaphore_signal(barrier, inc=1, device_id={"wav": peer}, device_id_type=MESH)
        return 0

    lax.fori_loop(1, wav_count, greet, 0)

    loads[0].wait()
    tail = jnp.zeros((block, 128), jnp.float32)
    for s in range(slots):
        at_row = lax.broadcasted_iota(jnp.int32, (rest, 128), 0)
        at_col = lax.broadcasted_iota(jnp.int32, (rest, 128), 1)
        place = (at_col == at_row + rest * s).astype(jnp.bfloat16)
        tail += jnp.dot(leg_ref[s, :, full:fold], place, preferred_element_type=jnp.float32)
    held[z, 0, 0] = tail.astype(jnp.bfloat16)
    for s in range(slots):
        for k in range(per_slot):
            i = 1 + s * per_slot + k
            held[z, i // chunk, i % chunk] = leg_ref[s, :, k * 128 : (k + 1) * 128]

    pl.semaphore_wait(barrier, 2 + wav_count - 1)

    half = lev_count // 2

    def goes(side, d, c):
        return d < half - 1 or c % 2 == side

    def hop(side, d, c):
        owner = lax.rem(z + (lev_count - d if side == 0 else d), lev_count)
        return pltpu.make_async_remote_copy(
            src_ref=held.at[owner, c],
            dst_ref=held.at[owner, c],
            send_sem=send_sem.at[side, d, c],
            recv_sem=recv_sem.at[side, d, c],
            device_id={"lev": right if side == 0 else left},
            device_id_type=MESH,
        )

    def arrived(side, d, c):
        owner = lax.rem(z + (lev_count - d - 1 if side == 0 else d + 1), lev_count)
        pltpu.make_async_remote_copy(
            src_ref=held.at[owner, c],
            dst_ref=held.at[owner, c],
            send_sem=send_sem.at[side, d, c],
            recv_sem=recv_sem.at[side, d, c],
            device_id={"lev": right if side == 0 else left},
            device_id_type=MESH,
        ).wait_recv()

    def step(d, c):
        for side in (0, 1):
            if d:
                arrived(side, d - 1, c)
            if goes(side, d, c):
                hop(side, d, c).start()

    landed = set()

    def last(c):
        if c not in landed:
            landed.add(c)
            arrived(c % 2, half - 1, c)

    def mask_slot(s):
        border = (fold - 1) - pair_ref[w * slots + s]
        at_row = lax.broadcasted_iota(jnp.int32, (128, rest), 0)
        at_col = lax.broadcasted_iota(jnp.int32, (128, rest), 1)
        place = (at_row == at_col + rest * s).astype(jnp.bfloat16)
        row = lax.broadcasted_iota(jnp.int32, (128, 128), 0)
        ending = jnp.dot(place, spec_ref[s, full:fold, :], preferred_element_type=jnp.float32)
        below = row - rest * s + full < border
        rhs[s, 0:128, 0:128] = jnp.where(below, ending, 0.0).astype(jnp.bfloat16)
        rhs[s, 0:128, 128:256] = jnp.where(below, 0.0, ending).astype(jnp.bfloat16)
        for k in range(per_slot):
            piece = spec_ref[s, k * 128 : (k + 1) * 128, :].astype(jnp.float32)
            below = row + k * 128 < border
            at = (k + 1) * 128
            rhs[s, at : at + 128, 0:128] = jnp.where(below, piece, 0.0).astype(jnp.bfloat16)
            rhs[s, at : at + 128, 128:256] = jnp.where(below, 0.0, piece).astype(jnp.bfloat16)

    def start_basis():
        pairs = pairs_ref[...].astype(jnp.float32)
        column[...] = jnp.transpose(jnp.broadcast_to(pairs, (128, total_slots)))
        for r in range(rows):
            for k in range(4):
                at = k * 256 + total_slots
                table[r, at : (k + 1) * 256, :] = jnp.zeros((256 - total_slots, WIDTH), jnp.bfloat16)

    strip = 32
    strips = total_slots // strip

    def basis_piece(i, _):
        r = lax.div(i, strips)
        first = pl.multiple_of(lax.rem(i, strips) * strip, strip)
        a = lat_ref[w * rows + r]
        lon = 20 + 4 * jnp.minimum(a, NLAT - 1 - a)
        highest = jnp.minimum(waves - 1, lax.shift_right_arithmetic(lon - 1, 1)).astype(jnp.float32)
        count = jnp.full((strip, 128), lon.astype(jnp.float32), jnp.float32)
        inverse = 1.0 / count
        lane = lax.broadcasted_iota(jnp.int32, (strip, 128), 1).astype(jnp.float32)
        pair = column[pl.ds(first, strip), :]
        for h in range(2):
            m = pair if h == 0 else (waves - 1.0) - pair
            weight = jnp.where(m == 0.0, 1.0, 2.0)
            weight = jnp.where((pair >= 0.0) & (m <= highest), weight, 0.0)
            minus = -2.0 * weight
            for c in range(WIDTH // 128):
                sin_half, cos_half = half_angle(m * (lane + 128.0 * c), count, inverse)
                scaled = sin_half * minus
                cos_part = (weight + scaled * sin_half).astype(jnp.bfloat16)
                sin_part = (scaled * cos_half).astype(jnp.bfloat16)
                table[r, pl.ds(h * 256 + first, strip), c * 128 : (c + 1) * 128] = cos_part
                table[r, pl.ds(512 + h * 256 + first, strip), c * 128 : (c + 1) * 128] = sin_part
        return 0

    made = [0]

    def more_basis(n):
        until = min(made[0] + n, rows * strips)
        if until > made[0]:
            lax.fori_loop(made[0], until, basis_piece, 0)
            made[0] = until

    def one_slot(s):
        parts = [0] + [1 + s * per_slot + k for k in range(per_slot)]
        for i in parts:
            last(i // chunk)
        total = None
        for a in range(0, len(parts), 2):
            pieces = [
                held[:, i // chunk, i % chunk].reshape(lev_count * block, 128) for i in parts[a : a + 2]
            ]
            lhs = jnp.concatenate(pieces, axis=1)
            term = jnp.dot(lhs, rhs[s, a * 128 : (a + 2) * 128], preferred_element_type=jnp.float32)
            total = term if total is None else total + term
        groups = total.reshape(wav_count, total.shape[0] // wav_count, 256)
        both = jnp.concatenate([groups[:, :, :128], groups[:, :, 128:]], axis=1)
        ready[s] = both.astype(jnp.bfloat16)

        def send(k, _):
            peer = lax.rem(w + k, wav_count)
            pltpu.make_async_remote_copy(
                src_ref=ready.at[s, peer],
                dst_ref=out_ref.at[w, s],
                send_sem=out_send,
                recv_sem=out_recv.at[w],
                device_id={"wav": peer},
                device_id_type=MESH,
            ).start()
            return 0

        lax.fori_loop(1, wav_count, send, 0)
        pltpu.make_async_copy(ready.at[s, w], out_ref.at[w, s], own_sem).start()

    for entry in order:
        kind, value = entry[0], entry[1:]
        if kind == "hop":
            step(*value)
        elif kind == "slot":
            one_slot(*value)
        elif kind == "basis":
            more_basis(*value)
        elif kind == "mask":
            loads[1].wait()
            loads[4].wait()
            for s in range(slots):
                mask_slot(s)
        else:
            loads[2].wait()
            loads[3].wait()
            start_basis()
    more_basis(rows * strips)
    finish = pltpu.make_async_copy(table, table_hbm, table_sem)
    finish.start()
    for c in range(chunks):
        last(c)

    for side in (0, 1):
        for d in range(half):
            for c in range(chunks):
                if goes(side, d, c):
                    hop(side, d, c).wait_send()

    finish.wait()
    pltpu.make_async_copy(out_ref.at[w], out_ref.at[w], own_sem).wait()
    pltpu.make_async_copy(ready.at[:, 1:], ready.at[:, 1:], out_send).wait()

    def arrival(k, _):
        peer = lax.rem(w + k, wav_count)
        pltpu.make_async_copy(out_ref.at[peer], out_ref.at[peer], out_recv.at[peer]).wait()
        return 0

    lax.fori_loop(1, wav_count, arrival, 0)


def plan(chunks, slots):
    early, late = list(range(5)), list(range(5, chunks))
    order = []

    def hops(d, which):
        order.extend(("hop", d, c) for c in which)

    hops(0, early)
    hops(0, late[:3])
    order.append(("mask",))
    hops(1, early)
    hops(0, late[3:])
    order.append(("start",))
    order.append(("basis", 12))
    hops(2, early)
    hops(1, late[:3])
    order.append(("basis", 14))
    hops(3, early)
    hops(1, late[3:])
    order.append(("basis", 16))
    hops(2, late[:3])
    order.append(("basis", 14))
    order.append(("slot", 0))
    hops(2, late[3:])
    order.append(("slot", 1))
    hops(3, late[:3])
    order.append(("slot", 2))
    hops(3, late[3:])
    order.extend(("slot", s) for s in range(3, slots))
    return order


def exchange(spectral, legendre, wave_pair, lat_slot):
    slots, fold, _ = spectral.shape
    wav_count = lax.axis_size("wav")
    lev_count = lax.axis_size("lev")
    block = legendre.shape[2]
    rows = block * lev_count // wav_count
    total = wave_pair.shape[0]
    turned = jnp.swapaxes(legendre, 1, 2)
    tiles = 1 + slots * (fold // 128)
    chunk = 2
    chunks = tiles // chunk
    half = lev_count // 2
    return pl.pallas_call(
        functools.partial(exchange_kernel, fold - 1, slots, fold, plan(chunks, slots)),
        out_shape=[
            jax.ShapeDtypeStruct((wav_count, slots, 2 * rows, 128), jnp.bfloat16),
            jax.ShapeDtypeStruct((rows, 1024, WIDTH), jnp.bfloat16),
        ],
        in_specs=[pl.BlockSpec(memory_space=pl.ANY)] * 5,
        out_specs=[pl.BlockSpec(memory_space=pl.ANY)] * 2,
        scratch_shapes=[
            pltpu.SMEM(wave_pair.shape, jnp.int32),
            pltpu.VMEM((1, total), jnp.int32),
            pltpu.SMEM(lat_slot.shape, jnp.int32),
            pltpu.VMEM(turned.shape, jnp.bfloat16),
            pltpu.VMEM(spectral.shape, jnp.bfloat16),
            pltpu.VMEM((lev_count, chunks, chunk, block, 128), jnp.bfloat16),
            pltpu.VMEM((slots, 512, 256), jnp.bfloat16),
            pltpu.VMEM((slots, wav_count, 2 * rows, 128), jnp.bfloat16),
            pltpu.VMEM((rows, 1024, WIDTH), jnp.bfloat16),
            pltpu.VMEM((total, 128), jnp.float32),
            pltpu.SemaphoreType.DMA((5,)),
            pltpu.SemaphoreType.DMA((2, half, chunks)),
            pltpu.SemaphoreType.DMA((2, half, chunks)),
            pltpu.SemaphoreType.DMA,
            pltpu.SemaphoreType.DMA((wav_count,)),
            pltpu.SemaphoreType.DMA,
            pltpu.SemaphoreType.DMA,
        ],
        compiler_params=pltpu.CompilerParams(collective_id=0, has_side_effects=True),
        name="exchange",
    )(wave_pair, wave_pair.reshape(1, total), lat_slot, turned, spectral)


def synthesis_kernel(waves, rows, pair_ref, lat_ref, in_ref, table, out_ref, flat, turned):
    r = pl.program_id(0)
    slots = pair_ref.shape[1]
    layers = out_ref.shape[1]
    width = out_ref.shape[2]
    blocks = (width + WIDTH - 1) // WIDTH

    @pl.when(r == 0)
    def _():
        flat[...] = in_ref[...].astype(jnp.float32)
        turned[...] = jnp.zeros_like(turned)

    a = lat_ref[lax.axis_index("wav") * rows + r]
    lon = 20 + 4 * jnp.minimum(a, NLAT - 1 - a)
    count = lon.astype(jnp.float32)
    target = lax.broadcasted_iota(jnp.int32, (128, 128), 0)
    source = lax.broadcasted_iota(jnp.int32, (128, 128), 1)
    part = (target >= layers).astype(jnp.int32)
    place = (source == 2 * (target - part * layers) + part).astype(jnp.bfloat16)
    count_row = jnp.full((8, slots), count, jnp.float32)
    inverse_row = 1.0 / count_row
    shift = lax.broadcasted_iota(jnp.int32, (8, slots), 0).astype(jnp.float32) * WIDTH
    for h in range(2):
        values = flat[pl.ds(h * rows + r, slots, stride=2 * rows), :].astype(jnp.bfloat16)
        split = lax.dot_general(
            place, values, (((1,), (1,)), ((), ())), preferred_element_type=jnp.float32
        )
        real, imag = split[:layers], split[layers:]
        pairs = jnp.broadcast_to(pair_ref[...].astype(jnp.float32), (8, slots))
        m = pairs if h == 0 else (waves - 1.0) - pairs
        sin_half, cos_half = half_angle(m * shift, count_row, inverse_row)
        sines = 2.0 * sin_half * cos_half
        cosines = 1.0 - 2.0 * sin_half * sin_half
        for b in range(blocks):
            at = pl.ds(b * layers, layers)
            if b == 0:
                turned_real, turned_imag = real, imag
            else:
                cos_b, sin_b = cosines[b : b + 1], sines[b : b + 1]
                turned_real = real * cos_b - imag * sin_b
                turned_imag = real * sin_b + imag * cos_b
            turned[at, h * 256 : h * 256 + slots] = turned_real.astype(jnp.bfloat16)
            turned[at, 512 + h * 256 : 512 + h * 256 + slots] = turned_imag.astype(jnp.bfloat16)

    result = jnp.dot(turned[...], table[0], preferred_element_type=jnp.float32)
    for b in range(blocks):
        size = min(WIDTH, width - b * WIDTH)
        col = lax.broadcasted_iota(jnp.int32, (layers, size), 1) + b * WIDTH
        piece = result[b * layers : (b + 1) * layers, :size]
        out_ref[0, :, b * WIDTH : b * WIDTH + size] = jnp.where(col < lon, piece, 0.0).astype(jnp.bfloat16)


def synthesis(received, table, wave_pair, lat_slot, waves):
    wav_count, slots, both, _ = received.shape
    rows = both // 2
    total = wav_count * slots
    layers = 64
    width = 2 * NLAT + 16
    blocks = (width + WIDTH - 1) // WIDTH
    flat = received.reshape(total * both, 128)
    return pl.pallas_call(
        functools.partial(synthesis_kernel, waves, rows),
        grid=(rows,),
        out_shape=jax.ShapeDtypeStruct((rows, layers, width), jnp.bfloat16),
        in_specs=[
            pl.BlockSpec((1, total), lambda r: (0, 0)),
            pl.BlockSpec(memory_space=pltpu.SMEM),
            pl.BlockSpec((total * both, 128), lambda r: (0, 0)),
            pl.BlockSpec((1, 1024, WIDTH), lambda r: (r, 0, 0)),
        ],
        out_specs=pl.BlockSpec((1, layers, width), lambda r: (r, 0, 0)),
        scratch_shapes=[
            pltpu.VMEM((total * both, 128), jnp.float32),
            pltpu.VMEM((blocks * layers, 1024), jnp.bfloat16),
        ],
        compiler_params=pltpu.CompilerParams(dimension_semantics=("arbitrary",)),
        name="synthesis",
    )(wave_pair.reshape(1, total), lat_slot, flat, table)


def on_device(spectral, legendre, wave_pair, lat_slot):
    received, table = exchange(spectral, legendre, wave_pair, lat_slot)
    return synthesis(received, table, wave_pair, lat_slot, spectral.shape[1] - 1)


def solution(mesh):
    return jax.shard_map(
        on_device,
        mesh=mesh,
        in_specs=(P("wav", None, "lev"), P("wav", None, "lev"), P(), P()),
        out_specs=P("wav", "lev", None),
        check_vma=False,
    )
```

```python
import functools

import jax
import jax.numpy as jnp
import numpy as np
from jax import lax
from jax.experimental import pallas as pl
from jax.experimental.pallas import tpu as pltpu
from jax.sharding import PartitionSpec as P

NLAT = 800
WIDTH = 256
PITCH = 24
MESH = pl.DeviceIdType.MESH


def poly_in_square(fn, degree):
    nodes = np.cos(np.pi * (np.arange(200) + 0.5) / 200)
    top = 0.52**2
    z = (nodes + 1) * 0.5 * top
    fit = np.polynomial.chebyshev.Chebyshev.fit(z, fn(np.sqrt(z)), degree, domain=[0, top])
    return [float(c) for c in fit.convert(kind=np.polynomial.Polynomial).coef]


SIN_COEF = poly_in_square(lambda x: np.sin(np.pi * x) / x, 5)
COS_COEF = poly_in_square(lambda x: np.cos(np.pi * x), 5)


def horner(coef, z):
    acc = jnp.full_like(z, coef[-1])
    for c in coef[-2::-1]:
        acc = acc * z + c
    return acc


def half_angle(steps, count, inverse):
    turns = jnp.floor(steps * inverse + 0.5)
    x = (steps - turns * count) * inverse
    z = x * x
    return x * horner(SIN_COEF, z), horner(COS_COEF, z)


def exchange_kernel(
    waves,
    slots,
    fold,
    order,
    pair_hbm,
    pairs_hbm,
    lat_hbm,
    leg_hbm,
    spec_hbm,
    out_ref,
    table_hbm,
    pair_ref,
    pairs_ref,
    lat_ref,
    leg_ref,
    spec_ref,
    held,
    rhs,
    ready,
    table,
    column,
    load_sem,
    send_sem,
    recv_sem,
    out_send,
    out_recv,
    own_sem,
    table_sem,
):
    wav_count = lax.axis_size("wav")
    lev_count = lax.axis_size("lev")
    w = lax.axis_index("wav")
    z = lax.axis_index("lev")
    right = lax.rem(z + 1, lev_count)
    left = lax.rem(z + lev_count - 1, lev_count)
    block = leg_ref.shape[1]
    full = (fold // 128) * 128
    rest = fold - full
    per_slot = full // 128
    chunks = held.shape[1]
    chunk = held.shape[2]
    rows = table.shape[0]
    total_slots = column.shape[0]

    sources = ((leg_hbm, leg_ref), (pair_hbm, pair_ref), (pairs_hbm, pairs_ref), (lat_hbm, lat_ref), (spec_hbm, spec_ref))
    loads = [pltpu.make_async_copy(src, dst, load_sem.at[i]) for i, (src, dst) in enumerate(sources)]
    for load in loads:
        load.start()

    barrier = pltpu.get_barrier_semaphore()
    for peer in (left, right):
        pl.semaphore_signal(barrier, inc=1, device_id={"lev": peer}, device_id_type=MESH)

    def greet(k, _):
        peer = lax.rem(w + k, wav_count)
        pl.semaphore_signal(barrier, inc=1, device_id={"wav": peer}, device_id_type=MESH)
        return 0

    lax.fori_loop(1, wav_count, greet, 0)

    loads[0].wait()
    tail = jnp.zeros((block, 128), jnp.float32)
    for s in range(slots):
        at_row = lax.broadcasted_iota(jnp.int32, (rest, 128), 0)
        at_col = lax.broadcasted_iota(jnp.int32, (rest, 128), 1)
        place = (at_col == at_row + rest * s).astype(jnp.bfloat16)
        tail += jnp.dot(leg_ref[s, :, full:fold], place, preferred_element_type=jnp.float32)
    held[z, 0, 0] = tail.astype(jnp.bfloat16)
    for s in range(slots):
        for k in range(per_slot):
            i = 1 + s * per_slot + k
            held[z, i // chunk, i % chunk] = leg_ref[s, :, k * 128 : (k + 1) * 128]

    pl.semaphore_wait(barrier, 2 + wav_count - 1)

    half = lev_count // 2

    def goes(side, d, c):
        return d < half - 1 or c % 2 == side

    def hop(side, d, c):
        owner = lax.rem(z + (lev_count - d if side == 0 else d), lev_count)
        return pltpu.make_async_remote_copy(
            src_ref=held.at[owner, c],
            dst_ref=held.at[owner, c],
            send_sem=send_sem.at[side, d, c],
            recv_sem=recv_sem.at[side, d, c],
            device_id={"lev": right if side == 0 else left},
            device_id_type=MESH,
        )

    def arrived(side, d, c):
        owner = lax.rem(z + (lev_count - d - 1 if side == 0 else d + 1), lev_count)
        pltpu.make_async_remote_copy(
            src_ref=held.at[owner, c],
            dst_ref=held.at[owner, c],
            send_sem=send_sem.at[side, d, c],
            recv_sem=recv_sem.at[side, d, c],
            device_id={"lev": right if side == 0 else left},
            device_id_type=MESH,
        ).wait_recv()

    def step(d, c):
        for side in (0, 1):
            if d:
                arrived(side, d - 1, c)
            if goes(side, d, c):
                hop(side, d, c).start()

    landed = set()

    def last(c):
        if c not in landed:
            landed.add(c)
            arrived(c % 2, half - 1, c)

    def mask_slot(s):
        border = (fold - 1) - pair_ref[w * slots + s]
        at_row = lax.broadcasted_iota(jnp.int32, (128, rest), 0)
        at_col = lax.broadcasted_iota(jnp.int32, (128, rest), 1)
        place = (at_row == at_col + rest * s).astype(jnp.bfloat16)
        row = lax.broadcasted_iota(jnp.int32, (128, 128), 0)
        ending = jnp.dot(place, spec_ref[s, full:fold, :], preferred_element_type=jnp.float32)
        below = row - rest * s + full < border
        rhs[s, 0:128, 0:128] = jnp.where(below, ending, 0.0).astype(jnp.bfloat16)
        rhs[s, 0:128, 128:256] = jnp.where(below, 0.0, ending).astype(jnp.bfloat16)
        for k in range(per_slot):
            piece = spec_ref[s, k * 128 : (k + 1) * 128, :].astype(jnp.float32)
            below = row + k * 128 < border
            at = (k + 1) * 128
            rhs[s, at : at + 128, 0:128] = jnp.where(below, piece, 0.0).astype(jnp.bfloat16)
            rhs[s, at : at + 128, 128:256] = jnp.where(below, 0.0, piece).astype(jnp.bfloat16)

    def start_basis():
        pairs = pairs_ref[...].astype(jnp.float32)
        column[...] = jnp.transpose(jnp.broadcast_to(pairs, (128, total_slots)))
        for r in range(rows):
            for k in range(4):
                at = k * 256 + total_slots
                for c in range(WIDTH // 128):
                    table[r, c, at : (k + 1) * 256, :] = jnp.zeros((256 - total_slots, 128), jnp.bfloat16)

    strip = 32
    strips = total_slots // strip

    def basis_piece(i, _):
        r = lax.div(i, strips)
        first = pl.multiple_of(lax.rem(i, strips) * strip, strip)
        a = lat_ref[w * rows + r]
        lon = 20 + 4 * jnp.minimum(a, NLAT - 1 - a)
        highest = jnp.minimum(waves - 1, lax.shift_right_arithmetic(lon - 1, 1)).astype(jnp.float32)
        count = jnp.full((strip, 128), lon.astype(jnp.float32), jnp.float32)
        inverse = 1.0 / count
        lane = lax.broadcasted_iota(jnp.int32, (strip, 128), 1).astype(jnp.float32)
        pair = column[pl.ds(first, strip), :]
        for h in range(2):
            m = pair if h == 0 else (waves - 1.0) - pair
            weight = jnp.where(m == 0.0, 1.0, 2.0)
            weight = jnp.where((pair >= 0.0) & (m <= highest), weight, 0.0)
            minus = -2.0 * weight
            for c in range(WIDTH // 128):
                sin_half, cos_half = half_angle(m * (lane + 128.0 * c), count, inverse)
                scaled = sin_half * minus
                cos_part = (weight + scaled * sin_half).astype(jnp.bfloat16)
                sin_part = (scaled * cos_half).astype(jnp.bfloat16)
                table[r, c, pl.ds(h * 256 + first, strip), :] = cos_part
                table[r, c, pl.ds(512 + h * 256 + first, strip), :] = sin_part
        return 0

    made = [0]

    def more_basis(n):
        until = min(made[0] + n, rows * strips)
        if until > made[0]:
            lax.fori_loop(made[0], until, basis_piece, 0)
            made[0] = until

    def one_slot(s):
        parts = [0] + [1 + s * per_slot + k for k in range(per_slot)]
        for i in parts:
            last(i // chunk)
        total = None
        for a in range(0, len(parts), 2):
            pieces = [
                held[:, i // chunk, i % chunk].reshape(lev_count * block, 128) for i in parts[a : a + 2]
            ]
            lhs = jnp.concatenate(pieces, axis=1)
            term = jnp.dot(lhs, rhs[s, a * 128 : (a + 2) * 128], preferred_element_type=jnp.float32)
            total = term if total is None else total + term
        groups = total.reshape(wav_count, total.shape[0] // wav_count, 256)
        both = jnp.concatenate([groups[:, :, :128], groups[:, :, 128:]], axis=1)
        ready[s] = both.astype(jnp.bfloat16)

        def send(k, _):
            peer = lax.rem(w + k, wav_count)
            pltpu.make_async_remote_copy(
                src_ref=ready.at[s, peer],
                dst_ref=out_ref.at[w, s],
                send_sem=out_send,
                recv_sem=out_recv.at[w],
                device_id={"wav": peer},
                device_id_type=MESH,
            ).start()
            return 0

        lax.fori_loop(1, wav_count, send, 0)
        pltpu.make_async_copy(ready.at[s, w], out_ref.at[w, s], own_sem).start()

    for entry in order:
        kind, value = entry[0], entry[1:]
        if kind == "hop":
            step(*value)
        elif kind == "slot":
            one_slot(*value)
        elif kind == "basis":
            more_basis(*value)
        elif kind == "mask":
            loads[1].wait()
            loads[4].wait()
            for s in range(slots):
                mask_slot(s)
        else:
            loads[2].wait()
            loads[3].wait()
            start_basis()
    more_basis(rows * strips)
    finish = pltpu.make_async_copy(table, table_hbm, table_sem)
    finish.start()
    for c in range(chunks):
        last(c)

    for side in (0, 1):
        for d in range(half):
            for c in range(chunks):
                if goes(side, d, c):
                    hop(side, d, c).wait_send()

    finish.wait()
    pltpu.make_async_copy(out_ref.at[w], out_ref.at[w], own_sem).wait()
    pltpu.make_async_copy(ready.at[:, 1:], ready.at[:, 1:], out_send).wait()

    def arrival(k, _):
        peer = lax.rem(w + k, wav_count)
        pltpu.make_async_copy(out_ref.at[peer], out_ref.at[peer], out_recv.at[peer]).wait()
        return 0

    lax.fori_loop(1, wav_count, arrival, 0)


def plan(slots):
    hops = [(0, c) for c in (0, 1, 2, 3, 8, 5, 10, 4, 6, 9)]
    order = [("hop", *hop) for hop in hops]
    order += [("mask",), ("start",), ("basis", 20)]
    later = [(1, 0), (1, 1), (1, 2), (0, 7), (1, 3), (1, 5), (1, 8), (1, 4), (1, 6), (1, 9), (2, 0), (2, 1)]
    later += [(1, 10), (2, 2), (2, 3), (2, 5), (1, 7), (2, 4), (2, 6), (3, 0), (2, 8), (3, 1), (2, 10), (3, 2)]
    later += [(2, 9), (3, 4), (3, 3), (3, 8), (3, 6), (2, 7), (3, 5)]
    for i, hop in enumerate(later):
        order.append(("hop", *hop))
        if i % 3 == 2:
            order.append(("basis", 4))
    order += [("slot", 0), ("hop", 3, 10), ("slot", 1), ("hop", 3, 7), ("hop", 3, 9)]
    return order + [("slot", s) for s in range(2, slots)]


def exchange(spectral, legendre, wave_pair, lat_slot):
    slots, fold, _ = spectral.shape
    wav_count = lax.axis_size("wav")
    lev_count = lax.axis_size("lev")
    block = legendre.shape[2]
    rows = block * lev_count // wav_count
    total = wave_pair.shape[0]
    turned = jnp.swapaxes(legendre, 1, 2)
    tiles = 1 + slots * (fold // 128)
    chunk = 2
    chunks = tiles // chunk
    half = lev_count // 2
    return pl.pallas_call(
        functools.partial(exchange_kernel, fold - 1, slots, fold, plan(slots)),
        out_shape=[
            jax.ShapeDtypeStruct((wav_count, slots, 2 * rows, 128), jnp.bfloat16),
            jax.ShapeDtypeStruct((rows, WIDTH // 128, 1024, 128), jnp.bfloat16),
        ],
        in_specs=[pl.BlockSpec(memory_space=pl.ANY)] * 5,
        out_specs=[pl.BlockSpec(memory_space=pl.ANY)] * 2,
        scratch_shapes=[
            pltpu.SMEM(wave_pair.shape, jnp.int32),
            pltpu.VMEM((1, total), jnp.int32),
            pltpu.SMEM(lat_slot.shape, jnp.int32),
            pltpu.VMEM(turned.shape, jnp.bfloat16),
            pltpu.VMEM(spectral.shape, jnp.bfloat16),
            pltpu.VMEM((lev_count, chunks, chunk, block, 128), jnp.bfloat16),
            pltpu.VMEM((slots, 512, 256), jnp.bfloat16),
            pltpu.VMEM((slots, wav_count, 2 * rows, 128), jnp.bfloat16),
            pltpu.VMEM((rows, WIDTH // 128, 1024, 128), jnp.bfloat16),
            pltpu.VMEM((total, 128), jnp.float32),
            pltpu.SemaphoreType.DMA((5,)),
            pltpu.SemaphoreType.DMA((2, half, chunks)),
            pltpu.SemaphoreType.DMA((2, half, chunks)),
            pltpu.SemaphoreType.DMA,
            pltpu.SemaphoreType.DMA((wav_count,)),
            pltpu.SemaphoreType.DMA,
            pltpu.SemaphoreType.DMA,
        ],
        compiler_params=pltpu.CompilerParams(collective_id=0, has_side_effects=True),
        name="exchange",
    )(wave_pair, wave_pair.reshape(1, total), lat_slot, turned, spectral)


def synthesis_kernel(waves, rows, together, pair_ref, lat_ref, in_ref, table, out_ref, flat, *turned):
    step = pl.program_id(0)
    slots = pair_ref.shape[1]
    layers = out_ref.shape[1]
    width = out_ref.shape[2]
    blocks = (width + WIDTH - 1) // WIDTH

    @pl.when(step == 0)
    def _():
        def unpack(i, _):
            values = in_ref[pl.ds(pl.multiple_of(i * 2 * rows, 2 * rows), 2 * rows), :]
            flat[pl.ds(pl.multiple_of(i * PITCH, 8), 2 * rows), :] = values.astype(jnp.float32)
            return 0

        lax.fori_loop(0, slots, unpack, 0, unroll=16)
        for buffer in turned:
            buffer[...] = jnp.zeros_like(buffer)

    target = lax.broadcasted_iota(jnp.int32, (128, 128), 0)
    source = lax.broadcasted_iota(jnp.int32, (128, 128), 1)
    part = (target >= layers).astype(jnp.int32)
    place = (source == 2 * (target - part * layers) + part).astype(jnp.bfloat16)
    shift = lax.broadcasted_iota(jnp.int32, (8, slots), 0).astype(jnp.float32) * WIDTH
    pairs = jnp.broadcast_to(pair_ref[...].astype(jnp.float32), (8, slots))
    lengths = []
    for i in range(together):
        r = step * together + i
        a = lat_ref[lax.axis_index("wav") * rows + r]
        lon = 20 + 4 * jnp.minimum(a, NLAT - 1 - a)
        lengths.append(lon)
        count = jnp.full((8, slots), lon.astype(jnp.float32), jnp.float32)
        inverse = 1.0 / count
        for h in range(2):
            values = flat[pl.ds(h * rows + r, slots, stride=PITCH), :].astype(jnp.bfloat16)
            split = lax.dot_general(
                place, values, (((1,), (1,)), ((), ())), preferred_element_type=jnp.float32
            )
            m = pairs if h == 0 else (waves - 1.0) - pairs
            sin_half, cos_half = half_angle(m * shift, count, inverse)
            sines = 2.0 * sin_half * cos_half
            cosines = 1.0 - 2.0 * sin_half * sin_half
            for k in range(2):
                lanes = slice(k * 128, min((k + 1) * 128, slots))
                size = lanes.stop - lanes.start
                real, imag = split[:layers, lanes], split[layers:, lanes]
                for b in range(blocks):
                    at = pl.ds(b * layers, layers)
                    if b == 0:
                        turned_real, turned_imag = real, imag
                    else:
                        cos_b, sin_b = cosines[b : b + 1, lanes], sines[b : b + 1, lanes]
                        turned_real = real * cos_b - imag * sin_b
                        turned_imag = real * sin_b + imag * cos_b
                    turned[i][2 * h + k, at, :size] = turned_real.astype(jnp.bfloat16)
                    turned[i][4 + 2 * h + k, at, :size] = turned_imag.astype(jnp.bfloat16)

    for i in range(together):
        lhs = jnp.concatenate([turned[i][k] for k in range(8)], axis=1)
        rhs = jnp.concatenate([table[i, c] for c in range(WIDTH // 128)], axis=1)
        result = jnp.dot(lhs, rhs, preferred_element_type=jnp.float32)
        for b in range(blocks):
            size = min(WIDTH, width - b * WIDTH)
            col = lax.broadcasted_iota(jnp.int32, (layers, size), 1) + b * WIDTH
            piece = result[b * layers : (b + 1) * layers, :size]
            piece = jnp.where(col < lengths[i], piece, 0.0).astype(jnp.bfloat16)
            out_ref[i, :, b * WIDTH : b * WIDTH + size] = piece


def synthesis(received, table, wave_pair, lat_slot, waves):
    wav_count, slots, both, _ = received.shape
    rows = both // 2
    total = wav_count * slots
    layers = 64
    width = 2 * NLAT + 16
    blocks = (width + WIDTH - 1) // WIDTH
    together = 2
    flat = received.reshape(total * both, 128)
    return pl.pallas_call(
        functools.partial(synthesis_kernel, waves, rows, together),
        grid=(rows // together,),
        out_shape=jax.ShapeDtypeStruct((rows, layers, width), jnp.bfloat16),
        in_specs=[
            pl.BlockSpec((1, total), lambda r: (0, 0)),
            pl.BlockSpec(memory_space=pltpu.SMEM),
            pl.BlockSpec((total * both, 128), lambda r: (0, 0)),
            pl.BlockSpec((together, WIDTH // 128, 1024, 128), lambda r: (r, 0, 0, 0)),
        ],
        out_specs=pl.BlockSpec((together, layers, width), lambda r: (r, 0, 0)),
        scratch_shapes=[
            pltpu.VMEM((total * PITCH, 128), jnp.float32),
        ]
        + [pltpu.VMEM((8, blocks * layers, 128), jnp.bfloat16)] * together,
        compiler_params=pltpu.CompilerParams(dimension_semantics=("arbitrary",)),
        name="synthesis",
    )(wave_pair.reshape(1, total), lat_slot, flat, table)


def on_device(spectral, legendre, wave_pair, lat_slot):
    received, table = exchange(spectral, legendre, wave_pair, lat_slot)
    return synthesis(received, table, wave_pair, lat_slot, spectral.shape[1] - 1)


def solution(mesh):
    return jax.shard_map(
        on_device,
        mesh=mesh,
        in_specs=(P("wav", None, "lev"), P("wav", None, "lev"), P(), P()),
        out_specs=P("wav", "lev", None),
        check_vma=False,
    )
```

```python
import functools

import jax
import jax.numpy as jnp
import numpy as np
from jax import lax
from jax.experimental import pallas as pl
from jax.experimental.pallas import tpu as pltpu
from jax.sharding import PartitionSpec as P

NLAT = 800
WIDTH = 256
PITCH = 24
GRANT = 20 * 2**20
MESH = pl.DeviceIdType.MESH


def poly_in_square(fn, degree):
    nodes = np.cos(np.pi * (np.arange(200) + 0.5) / 200)
    top = 0.52**2
    z = (nodes + 1) * 0.5 * top
    fit = np.polynomial.chebyshev.Chebyshev.fit(z, fn(np.sqrt(z)), degree, domain=[0, top])
    return [float(c) for c in fit.convert(kind=np.polynomial.Polynomial).coef]


SIN_COEF = poly_in_square(lambda x: np.sin(np.pi * x) / x, 5)
COS_COEF = poly_in_square(lambda x: np.cos(np.pi * x), 5)


def horner(coef, z):
    acc = jnp.full_like(z, coef[-1])
    for c in coef[-2::-1]:
        acc = acc * z + c
    return acc


def half_angle(steps, count, inverse):
    turns = jnp.floor(steps * inverse + 0.5)
    x = (steps - turns * count) * inverse
    z = x * x
    return x * horner(SIN_COEF, z), horner(COS_COEF, z)


def exchange_kernel(
    waves,
    slots,
    fold,
    order,
    pair_hbm,
    pairs_hbm,
    lat_hbm,
    leg_hbm,
    spec_hbm,
    out_ref,
    table,
    pair_ref,
    pairs_ref,
    lat_ref,
    leg_ref,
    spec_ref,
    held,
    rhs,
    ready,
    column,
    load_sem,
    send_sem,
    recv_sem,
    out_send,
    out_recv,
):
    wav_count = lax.axis_size("wav")
    lev_count = lax.axis_size("lev")
    w = lax.axis_index("wav")
    z = lax.axis_index("lev")
    right = lax.rem(z + 1, lev_count)
    left = lax.rem(z + lev_count - 1, lev_count)
    block = leg_ref.shape[1]
    full = (fold // 128) * 128
    rest = fold - full
    per_slot = full // 128
    chunks = held.shape[1]
    chunk = held.shape[2]
    rows = table.shape[0]
    total_slots = column.shape[0]

    sources = ((leg_hbm, leg_ref), (pair_hbm, pair_ref), (pairs_hbm, pairs_ref), (lat_hbm, lat_ref), (spec_hbm, spec_ref))
    loads = [pltpu.make_async_copy(src, dst, load_sem.at[i]) for i, (src, dst) in enumerate(sources)]
    for load in loads:
        load.start()

    barrier = pltpu.get_barrier_semaphore()
    for peer in (left, right):
        pl.semaphore_signal(barrier, inc=1, device_id={"lev": peer}, device_id_type=MESH)

    def greet(k, _):
        peer = lax.rem(w + k, wav_count)
        pl.semaphore_signal(barrier, inc=1, device_id={"wav": peer}, device_id_type=MESH)
        return 0

    lax.fori_loop(1, wav_count, greet, 0)

    loads[0].wait()
    tail = jnp.zeros((block, 128), jnp.float32)
    for s in range(slots):
        at_row = lax.broadcasted_iota(jnp.int32, (rest, 128), 0)
        at_col = lax.broadcasted_iota(jnp.int32, (rest, 128), 1)
        place = (at_col == at_row + rest * s).astype(jnp.bfloat16)
        tail += jnp.dot(leg_ref[s, :, full:fold], place, preferred_element_type=jnp.float32)
    held[z, 0, 0] = tail.astype(jnp.bfloat16)
    for s in range(slots):
        for k in range(per_slot):
            i = 1 + s * per_slot + k
            held[z, i // chunk, i % chunk] = leg_ref[s, :, k * 128 : (k + 1) * 128]

    pl.semaphore_wait(barrier, 2 + wav_count - 1)

    half = lev_count // 2

    def goes(side, d, c):
        return d < half - 1 or c % 2 == side

    def hop(side, d, c):
        owner = lax.rem(z + (lev_count - d if side == 0 else d), lev_count)
        return pltpu.make_async_remote_copy(
            src_ref=held.at[owner, c],
            dst_ref=held.at[owner, c],
            send_sem=send_sem.at[side, d, c],
            recv_sem=recv_sem.at[side, d, c],
            device_id={"lev": right if side == 0 else left},
            device_id_type=MESH,
        )

    def arrived(side, d, c):
        owner = lax.rem(z + (lev_count - d - 1 if side == 0 else d + 1), lev_count)
        pltpu.make_async_remote_copy(
            src_ref=held.at[owner, c],
            dst_ref=held.at[owner, c],
            send_sem=send_sem.at[side, d, c],
            recv_sem=recv_sem.at[side, d, c],
            device_id={"lev": right if side == 0 else left},
            device_id_type=MESH,
        ).wait_recv()

    def step(d, c):
        for side in (0, 1):
            if d:
                arrived(side, d - 1, c)
            if goes(side, d, c):
                hop(side, d, c).start()

    landed = set()

    def last(c):
        if c not in landed:
            landed.add(c)
            arrived(c % 2, half - 1, c)

    def mask_slot(s):
        border = (fold - 1) - pair_ref[w * slots + s]
        at_row = lax.broadcasted_iota(jnp.int32, (128, rest), 0)
        at_col = lax.broadcasted_iota(jnp.int32, (128, rest), 1)
        place = (at_row == at_col + rest * s).astype(jnp.bfloat16)
        row = lax.broadcasted_iota(jnp.int32, (128, 128), 0)
        ending = jnp.dot(place, spec_ref[s, full:fold, :], preferred_element_type=jnp.float32)
        below = row - rest * s + full < border
        rhs[s, 0:128, 0:128] = jnp.where(below, ending, 0.0).astype(jnp.bfloat16)
        rhs[s, 0:128, 128:256] = jnp.where(below, 0.0, ending).astype(jnp.bfloat16)
        for k in range(per_slot):
            piece = spec_ref[s, k * 128 : (k + 1) * 128, :].astype(jnp.float32)
            below = row + k * 128 < border
            at = (k + 1) * 128
            rhs[s, at : at + 128, 0:128] = jnp.where(below, piece, 0.0).astype(jnp.bfloat16)
            rhs[s, at : at + 128, 128:256] = jnp.where(below, 0.0, piece).astype(jnp.bfloat16)

    def start_basis():
        pairs = pairs_ref[...].astype(jnp.float32)
        column[...] = jnp.transpose(jnp.broadcast_to(pairs, (128, total_slots)))
        for r in range(rows):
            for k in range(4):
                at = k * 256 + total_slots
                for c in range(WIDTH // 128):
                    table[r, c, at : (k + 1) * 256, :] = jnp.zeros((256 - total_slots, 128), jnp.bfloat16)

    strip = 32
    strips = total_slots // strip

    def basis_piece(i, _):
        r = lax.div(i, strips)
        first = pl.multiple_of(lax.rem(i, strips) * strip, strip)
        a = lat_ref[w * rows + r]
        lon = 20 + 4 * jnp.minimum(a, NLAT - 1 - a)
        highest = jnp.minimum(waves - 1, lax.shift_right_arithmetic(lon - 1, 1)).astype(jnp.float32)
        count = jnp.full((strip, 128), lon.astype(jnp.float32), jnp.float32)
        inverse = 1.0 / count
        lane = lax.broadcasted_iota(jnp.int32, (strip, 128), 1).astype(jnp.float32)
        pair = column[pl.ds(first, strip), :]
        for h in range(2):
            m = pair if h == 0 else (waves - 1.0) - pair
            weight = jnp.where(m == 0.0, 1.0, 2.0)
            weight = jnp.where((pair >= 0.0) & (m <= highest), weight, 0.0)
            minus = -2.0 * weight
            for c in range(WIDTH // 128):
                sin_half, cos_half = half_angle(m * (lane + 128.0 * c), count, inverse)
                scaled = sin_half * minus
                cos_part = (weight + scaled * sin_half).astype(jnp.bfloat16)
                sin_part = (scaled * cos_half).astype(jnp.bfloat16)
                table[r, c, pl.ds(h * 256 + first, strip), :] = cos_part
                table[r, c, pl.ds(512 + h * 256 + first, strip), :] = sin_part
        return 0

    made = [0]

    def more_basis(n):
        until = min(made[0] + n, rows * strips)
        if until > made[0]:
            lax.fori_loop(made[0], until, basis_piece, 0)
            made[0] = until

    def one_slot(s):
        parts = [0] + [1 + s * per_slot + k for k in range(per_slot)]
        for i in parts:
            last(i // chunk)
        total = None
        for a in range(0, len(parts), 2):
            pieces = [
                held[:, i // chunk, i % chunk].reshape(lev_count * block, 128) for i in parts[a : a + 2]
            ]
            lhs = jnp.concatenate(pieces, axis=1)
            term = jnp.dot(lhs, rhs[s, a * 128 : (a + 2) * 128], preferred_element_type=jnp.float32)
            total = term if total is None else total + term
        groups = total.reshape(wav_count, total.shape[0] // wav_count, 256)
        both = jnp.concatenate([groups[:, :, :128], groups[:, :, 128:]], axis=1)
        ready[s] = both.astype(jnp.bfloat16)

        def send(k, _):
            peer = lax.rem(w + k, wav_count)
            pltpu.make_async_remote_copy(
                src_ref=ready.at[s, peer],
                dst_ref=out_ref.at[w, s],
                send_sem=out_send,
                recv_sem=out_recv.at[w],
                device_id={"wav": peer},
                device_id_type=MESH,
            ).start()
            return 0

        lax.fori_loop(1, wav_count, send, 0)
        out_ref[w, s] = ready[s, w]

    for entry in order:
        kind, value = entry[0], entry[1:]
        if kind == "hop":
            step(*value)
        elif kind == "slot":
            one_slot(*value)
        elif kind == "basis":
            more_basis(*value)
        elif kind == "mask":
            loads[1].wait()
            loads[4].wait()
            for s in range(slots):
                mask_slot(s)
        else:
            loads[2].wait()
            loads[3].wait()
            start_basis()
    more_basis(rows * strips)
    for c in range(chunks):
        last(c)

    for side in (0, 1):
        for d in range(half):
            for c in range(chunks):
                if goes(side, d, c):
                    hop(side, d, c).wait_send()

    pltpu.make_async_copy(ready.at[:, 1:], ready.at[:, 1:], out_send).wait()

    def arrival(k, _):
        peer = lax.rem(w + k, wav_count)
        pltpu.make_async_copy(out_ref.at[peer], out_ref.at[peer], out_recv.at[peer]).wait()
        return 0

    lax.fori_loop(1, wav_count, arrival, 0)


def plan(slots):
    hops = [(0, c) for c in (0, 1, 2, 3, 8, 5, 10, 4, 6, 9)]
    order = [("hop", *hop) for hop in hops]
    order += [("mask",), ("start",), ("basis", 20)]
    later = [(1, 0), (1, 1), (1, 2), (0, 7), (1, 3), (1, 5), (1, 8), (1, 4), (1, 6), (1, 9), (2, 0), (2, 1)]
    later += [(1, 10), (2, 2), (2, 3), (2, 5), (1, 7), (2, 4), (2, 6), (3, 0), (2, 8), (3, 1), (2, 10), (3, 2)]
    later += [(2, 9), (3, 4), (3, 3), (3, 8), (3, 6), (2, 7), (3, 5)]
    for i, hop in enumerate(later):
        order.append(("hop", *hop))
        if i % 3 == 2:
            order.append(("basis", 4))
    order += [("slot", 0), ("hop", 3, 10), ("slot", 1), ("hop", 3, 7), ("hop", 3, 9)]
    return order + [("slot", s) for s in range(2, slots)]


def exchange(spectral, legendre, wave_pair, lat_slot):
    slots, fold, _ = spectral.shape
    wav_count = lax.axis_size("wav")
    lev_count = lax.axis_size("lev")
    block = legendre.shape[2]
    rows = block * lev_count // wav_count
    total = wave_pair.shape[0]
    turned = jnp.swapaxes(legendre, 1, 2)
    tiles = 1 + slots * (fold // 128)
    chunk = 2
    chunks = tiles // chunk
    half = lev_count // 2
    return pl.pallas_call(
        functools.partial(exchange_kernel, fold - 1, slots, fold, plan(slots)),
        out_shape=[
            jax.ShapeDtypeStruct((wav_count, slots, 2 * rows, 128), jnp.bfloat16),
            jax.ShapeDtypeStruct((rows, WIDTH // 128, 1024, 128), jnp.bfloat16),
        ],
        in_specs=[pl.BlockSpec(memory_space=pltpu.HBM)] * 5,
        out_specs=[pl.BlockSpec(memory_space=pltpu.VMEM)] * 2,
        scratch_shapes=[
            pltpu.SMEM(wave_pair.shape, jnp.int32),
            pltpu.VMEM((1, total), jnp.int32),
            pltpu.SMEM(lat_slot.shape, jnp.int32),
            pltpu.VMEM(turned.shape, jnp.bfloat16),
            pltpu.VMEM(spectral.shape, jnp.bfloat16),
            pltpu.VMEM((lev_count, chunks, chunk, block, 128), jnp.bfloat16),
            pltpu.VMEM((slots, 512, 256), jnp.bfloat16),
            pltpu.VMEM((slots, wav_count, 2 * rows, 128), jnp.bfloat16),
            pltpu.VMEM((total, 128), jnp.float32),
            pltpu.SemaphoreType.DMA((5,)),
            pltpu.SemaphoreType.DMA((2, half, chunks)),
            pltpu.SemaphoreType.DMA((2, half, chunks)),
            pltpu.SemaphoreType.DMA,
            pltpu.SemaphoreType.DMA((wav_count,)),
        ],
        compiler_params=pltpu.CompilerParams(
            collective_id=0, has_side_effects=True, vmem_limit_bytes=GRANT
        ),
        name="exchange",
    )(*(pltpu.with_memory_space_constraint(x, pltpu.HBM) for x in (wave_pair, wave_pair.reshape(1, total), lat_slot, turned, spectral)))


def synthesis_kernel(waves, rows, together, pair_ref, lat_ref, in_ref, table, out_ref, flat, *turned):
    step = pl.program_id(0)
    slots = pair_ref.shape[1]
    layers = out_ref.shape[1]
    width = out_ref.shape[2]
    blocks = (width + WIDTH - 1) // WIDTH

    @pl.when(step == 0)
    def _():
        def unpack(i, _):
            values = in_ref[pl.ds(pl.multiple_of(i * 2 * rows, 2 * rows), 2 * rows), :]
            flat[pl.ds(pl.multiple_of(i * PITCH, 8), 2 * rows), :] = values.astype(jnp.float32)
            return 0

        lax.fori_loop(0, slots, unpack, 0, unroll=16)
        for buffer in turned:
            buffer[...] = jnp.zeros_like(buffer)

    target = lax.broadcasted_iota(jnp.int32, (128, 128), 0)
    source = lax.broadcasted_iota(jnp.int32, (128, 128), 1)
    part = (target >= layers).astype(jnp.int32)
    place = (source == 2 * (target - part * layers) + part).astype(jnp.bfloat16)
    shift = lax.broadcasted_iota(jnp.int32, (8, slots), 0).astype(jnp.float32) * WIDTH
    pairs = jnp.broadcast_to(pair_ref[...].astype(jnp.float32), (8, slots))
    lengths = []
    for i in range(together):
        r = step * together + i
        a = lat_ref[lax.axis_index("wav") * rows + r]
        lon = 20 + 4 * jnp.minimum(a, NLAT - 1 - a)
        lengths.append(lon)
        count = jnp.full((8, slots), lon.astype(jnp.float32), jnp.float32)
        inverse = 1.0 / count
        for h in range(2):
            values = flat[pl.ds(h * rows + r, slots, stride=PITCH), :].astype(jnp.bfloat16)
            split = lax.dot_general(
                place, values, (((1,), (1,)), ((), ())), preferred_element_type=jnp.float32
            )
            m = pairs if h == 0 else (waves - 1.0) - pairs
            sin_half, cos_half = half_angle(m * shift, count, inverse)
            sines = 2.0 * sin_half * cos_half
            cosines = 1.0 - 2.0 * sin_half * sin_half
            for k in range(2):
                lanes = slice(k * 128, min((k + 1) * 128, slots))
                size = lanes.stop - lanes.start
                real, imag = split[:layers, lanes], split[layers:, lanes]
                for b in range(blocks):
                    at = pl.ds(b * layers, layers)
                    if b == 0:
                        turned_real, turned_imag = real, imag
                    else:
                        cos_b, sin_b = cosines[b : b + 1, lanes], sines[b : b + 1, lanes]
                        turned_real = real * cos_b - imag * sin_b
                        turned_imag = real * sin_b + imag * cos_b
                    turned[i][2 * h + k, at, :size] = turned_real.astype(jnp.bfloat16)
                    turned[i][4 + 2 * h + k, at, :size] = turned_imag.astype(jnp.bfloat16)

    for i in range(together):
        lhs = jnp.concatenate([turned[i][k] for k in range(8)], axis=1)
        rhs = jnp.concatenate([table[i, c] for c in range(WIDTH // 128)], axis=1)
        result = jnp.dot(lhs, rhs, preferred_element_type=jnp.float32)
        for b in range(blocks):
            size = min(WIDTH, width - b * WIDTH)
            col = lax.broadcasted_iota(jnp.int32, (layers, size), 1) + b * WIDTH
            piece = result[b * layers : (b + 1) * layers, :size]
            piece = jnp.where(col < lengths[i], piece, 0.0).astype(jnp.bfloat16)
            out_ref[i, :, b * WIDTH : b * WIDTH + size] = piece


def synthesis(received, table, wave_pair, lat_slot, waves):
    wav_count, slots, both, _ = received.shape
    rows = both // 2
    total = wav_count * slots
    layers = 64
    width = 2 * NLAT + 16
    blocks = (width + WIDTH - 1) // WIDTH
    together = 2
    flat = received.reshape(total * both, 128)
    return pl.pallas_call(
        functools.partial(synthesis_kernel, waves, rows, together),
        grid=(rows // together,),
        out_shape=jax.ShapeDtypeStruct((rows, layers, width), jnp.bfloat16),
        in_specs=[
            pl.BlockSpec((1, total), lambda r: (0, 0)),
            pl.BlockSpec(memory_space=pltpu.SMEM),
            pl.BlockSpec((total * both, 128), lambda r: (0, 0)),
            pl.BlockSpec((together, WIDTH // 128, 1024, 128), lambda r: (r, 0, 0, 0)),
        ],
        out_specs=pl.BlockSpec((together, layers, width), lambda r: (r, 0, 0)),
        scratch_shapes=[
            pltpu.VMEM((total * PITCH, 128), jnp.float32),
        ]
        + [pltpu.VMEM((8, blocks * layers, 128), jnp.bfloat16)] * together,
        compiler_params=pltpu.CompilerParams(
            dimension_semantics=("arbitrary",), vmem_limit_bytes=GRANT
        ),
        name="synthesis",
    )(wave_pair.reshape(1, total), lat_slot, flat, table)


def on_device(spectral, legendre, wave_pair, lat_slot):
    received, table = exchange(spectral, legendre, wave_pair, lat_slot)
    return synthesis(received, table, wave_pair, lat_slot, spectral.shape[1] - 1)


def solution(mesh):
    return jax.shard_map(
        on_device,
        mesh=mesh,
        in_specs=(P("wav", None, "lev"), P("wav", None, "lev"), P(), P()),
        out_specs=P("wav", "lev", None),
        check_vma=False,
    )
```

```python
import functools

import jax
import jax.numpy as jnp
import numpy as np
from jax import lax
from jax.experimental import pallas as pl
from jax.experimental.pallas import tpu as pltpu
from jax.sharding import PartitionSpec as P

NLAT = 800
WIDTH = 256
PITCH = 24
EARLY = 3
GRANT = 20 * 2**20
MESH = pl.DeviceIdType.MESH


def poly_in_square(fn, degree):
    nodes = np.cos(np.pi * (np.arange(200) + 0.5) / 200)
    top = 0.52**2
    z = (nodes + 1) * 0.5 * top
    fit = np.polynomial.chebyshev.Chebyshev.fit(z, fn(np.sqrt(z)), degree, domain=[0, top])
    return [float(c) for c in fit.convert(kind=np.polynomial.Polynomial).coef]


SIN_COEF = poly_in_square(lambda x: np.sin(np.pi * x) / x, 5)
COS_COEF = poly_in_square(lambda x: np.cos(np.pi * x), 5)


def horner(coef, z):
    acc = jnp.full_like(z, coef[-1])
    for c in coef[-2::-1]:
        acc = acc * z + c
    return acc


def half_angle(steps, count, inverse):
    turns = jnp.floor(steps * inverse + 0.5)
    x = (steps - turns * count) * inverse
    z = x * x
    return x * horner(SIN_COEF, z), horner(COS_COEF, z)


def lined_up(pairs, first, past, wav_count, slots):
    lanes = 4 * wav_count
    index = lax.broadcasted_iota(jnp.int32, (pairs.shape[1], lanes), 0)
    lane = lax.broadcasted_iota(jnp.int32, (pairs.shape[1], lanes), 1)
    local = first + lax.div(lane, wav_count)
    chosen = (index == lax.rem(lane, wav_count) * slots + local) & (local < past)
    shifted = jnp.broadcast_to(pairs + 1.0, (16, pairs.shape[1])).astype(jnp.bfloat16)
    return jnp.dot(shifted, chosen.astype(jnp.bfloat16), preferred_element_type=jnp.float32)[:8] - 1.0


def unpack(flat, source, count, both):
    def piece(i, _):
        values = source[pl.ds(pl.multiple_of(i * both, both), both), :]
        flat[pl.ds(pl.multiple_of(i * PITCH, 8), both), :] = values.astype(jnp.float32)
        return 0

    lax.fori_loop(0, count, piece, 0, unroll=16)


def turn_row(waves, rows, layers, blocks, count, pairs, flat, r, lon, turned):
    target = lax.broadcasted_iota(jnp.int32, (128, 128), 0)
    source = lax.broadcasted_iota(jnp.int32, (128, 128), 1)
    part = (target >= layers).astype(jnp.int32)
    place = (source == 2 * (target - part * layers) + part).astype(jnp.bfloat16)
    shift = lax.broadcasted_iota(jnp.int32, (8, count), 0).astype(jnp.float32) * WIDTH
    points = jnp.full((8, count), lon.astype(jnp.float32), jnp.float32)
    inverse = 1.0 / points
    for h in range(2):
        values = flat[pl.ds(h * rows + r, count, stride=PITCH), :].astype(jnp.bfloat16)
        split = lax.dot_general(place, values, (((1,), (1,)), ((), ())), preferred_element_type=jnp.float32)
        real, imag = split[:layers], split[layers:]
        m = pairs[:, :count] if h == 0 else (waves - 1.0) - pairs[:, :count]
        sin_half, cos_half = half_angle(m * shift, points, inverse)
        sines = 2.0 * sin_half * cos_half
        cosines = 1.0 - 2.0 * sin_half * sin_half
        for b in range(blocks):
            at = pl.ds(b * layers, layers)
            if b == 0:
                turned_real, turned_imag = real, imag
            else:
                cos_b, sin_b = cosines[b : b + 1], sines[b : b + 1]
                turned_real = real * cos_b - imag * sin_b
                turned_imag = real * sin_b + imag * cos_b
            turned[h, at, :count] = turned_real.astype(jnp.bfloat16)
            turned[2 + h, at, :count] = turned_imag.astype(jnp.bfloat16)


def multiply(turned, columns):
    lhs = jnp.concatenate([turned[k] for k in range(4)], axis=1)
    return jnp.dot(lhs, jnp.concatenate(columns, axis=1), preferred_element_type=jnp.float32)


def longitudes(latitude):
    return 20 + 4 * jnp.minimum(latitude, NLAT - 1 - latitude)


def exchange_kernel(
    waves,
    slots,
    fold,
    order,
    pair_hbm,
    pairs_hbm,
    lat_hbm,
    leg_hbm,
    spec_hbm,
    late_ref,
    table,
    sums,
    pair_ref,
    pairs_ref,
    lat_ref,
    leg_ref,
    spec_ref,
    held,
    rhs,
    ready,
    column,
    lanes,
    early,
    flat,
    turned,
    load_sem,
    send_sem,
    recv_sem,
    out_send,
    out_recv,
):
    wav_count = lax.axis_size("wav")
    lev_count = lax.axis_size("lev")
    w = lax.axis_index("wav")
    z = lax.axis_index("lev")
    right = lax.rem(z + 1, lev_count)
    left = lax.rem(z + lev_count - 1, lev_count)
    block = leg_ref.shape[1]
    full = (fold // 128) * 128
    rest = fold - full
    per_slot = full // 128
    chunks = held.shape[1]
    chunk = held.shape[2]
    rows = table.shape[1]
    total_slots = column.shape[0]

    sources = ((leg_hbm, leg_ref), (pair_hbm, pair_ref), (pairs_hbm, pairs_ref), (lat_hbm, lat_ref), (spec_hbm, spec_ref))
    loads = [pltpu.make_async_copy(src, dst, load_sem.at[i]) for i, (src, dst) in enumerate(sources)]
    for load in loads:
        load.start()

    barrier = pltpu.get_barrier_semaphore()
    for peer in (left, right):
        pl.semaphore_signal(barrier, inc=1, device_id={"lev": peer}, device_id_type=MESH)

    def greet(k, _):
        peer = lax.rem(w + k, wav_count)
        pl.semaphore_signal(barrier, inc=1, device_id={"wav": peer}, device_id_type=MESH)
        return 0

    lax.fori_loop(1, wav_count, greet, 0)

    loads[0].wait()
    tail = jnp.zeros((block, 128), jnp.float32)
    for s in range(slots):
        at_row = lax.broadcasted_iota(jnp.int32, (rest, 128), 0)
        at_col = lax.broadcasted_iota(jnp.int32, (rest, 128), 1)
        place = (at_col == at_row + rest * s).astype(jnp.bfloat16)
        tail += jnp.dot(leg_ref[s, :, full:fold], place, preferred_element_type=jnp.float32)
    held[z, 0, 0] = tail.astype(jnp.bfloat16)
    for s in range(slots):
        for k in range(per_slot):
            i = 1 + s * per_slot + k
            held[z, i // chunk, i % chunk] = leg_ref[s, :, k * 128 : (k + 1) * 128]

    pl.semaphore_wait(barrier, 2 + wav_count - 1)

    half = lev_count // 2

    def goes(side, d, c):
        return d < half - 1 or c % 2 == side

    def hop(side, d, c):
        owner = lax.rem(z + (lev_count - d if side == 0 else d), lev_count)
        return pltpu.make_async_remote_copy(
            src_ref=held.at[owner, c],
            dst_ref=held.at[owner, c],
            send_sem=send_sem.at[side, d, c],
            recv_sem=recv_sem.at[side, d, c],
            device_id={"lev": right if side == 0 else left},
            device_id_type=MESH,
        )

    def arrived(side, d, c):
        owner = lax.rem(z + (lev_count - d - 1 if side == 0 else d + 1), lev_count)
        pltpu.make_async_remote_copy(
            src_ref=held.at[owner, c],
            dst_ref=held.at[owner, c],
            send_sem=send_sem.at[side, d, c],
            recv_sem=recv_sem.at[side, d, c],
            device_id={"lev": right if side == 0 else left},
            device_id_type=MESH,
        ).wait_recv()

    def step(d, c):
        for side in (0, 1):
            if d:
                arrived(side, d - 1, c)
            if goes(side, d, c):
                hop(side, d, c).start()

    landed = set()

    def last(c):
        if c not in landed:
            landed.add(c)
            arrived(c % 2, half - 1, c)

    def mask_slot(s):
        border = (fold - 1) - pair_ref[w * slots + s]
        at_row = lax.broadcasted_iota(jnp.int32, (128, rest), 0)
        at_col = lax.broadcasted_iota(jnp.int32, (128, rest), 1)
        place = (at_row == at_col + rest * s).astype(jnp.bfloat16)
        row = lax.broadcasted_iota(jnp.int32, (128, 128), 0)
        ending = jnp.dot(place, spec_ref[s, full:fold, :], preferred_element_type=jnp.float32)
        below = row - rest * s + full < border
        rhs[s, 0:128, 0:128] = jnp.where(below, ending, 0.0).astype(jnp.bfloat16)
        rhs[s, 0:128, 128:256] = jnp.where(below, 0.0, ending).astype(jnp.bfloat16)
        for k in range(per_slot):
            piece = spec_ref[s, k * 128 : (k + 1) * 128, :].astype(jnp.float32)
            below = row + k * 128 < border
            at = (k + 1) * 128
            rhs[s, at : at + 128, 0:128] = jnp.where(below, piece, 0.0).astype(jnp.bfloat16)
            rhs[s, at : at + 128, 128:256] = jnp.where(below, 0.0, piece).astype(jnp.bfloat16)

    def start_basis():
        pairs = pairs_ref[...].astype(jnp.float32)
        for g in range(2):
            lined = lined_up(pairs, EARLY * g, slots if g else EARLY, wav_count, slots)
            lanes[:, g * 128 : (g + 1) * 128] = lined
            column[g * 128 : (g + 1) * 128, :] = jnp.transpose(jnp.broadcast_to(lined[:1], (128, 128)))

    strip = 32
    strips = total_slots // strip

    def basis_piece(i, _):
        r = lax.div(i, strips)
        block_of = lax.rem(i, strips)
        first = pl.multiple_of(block_of * strip, strip)
        group = lax.div(block_of, 4)
        local = pl.multiple_of(lax.rem(block_of, 4) * strip, strip)
        lon = longitudes(lat_ref[w * rows + r])
        highest = jnp.minimum(waves - 1, lax.shift_right_arithmetic(lon - 1, 1)).astype(jnp.float32)
        count = jnp.full((strip, 128), lon.astype(jnp.float32), jnp.float32)
        inverse = 1.0 / count
        lane = lax.broadcasted_iota(jnp.int32, (strip, 128), 1).astype(jnp.float32)
        pair = column[pl.ds(first, strip), :]
        for h in range(2):
            m = pair if h == 0 else (waves - 1.0) - pair
            weight = jnp.where(m == 0.0, 1.0, 2.0)
            weight = jnp.where((pair >= 0.0) & (m <= highest), weight, 0.0)
            minus = -2.0 * weight
            for c in range(WIDTH // 128):
                sin_half, cos_half = half_angle(m * (lane + 128.0 * c), count, inverse)
                scaled = sin_half * minus
                cos_part = (weight + scaled * sin_half).astype(jnp.bfloat16)
                sin_part = (scaled * cos_half).astype(jnp.bfloat16)
                table[group, r, c, pl.ds(h * 128 + local, strip), :] = cos_part
                table[group, r, c, pl.ds(256 + h * 128 + local, strip), :] = sin_part
        return 0

    made = [0]

    def more_basis(n):
        until = min(made[0] + n, rows * strips)
        if until > made[0]:
            lax.fori_loop(made[0], until, basis_piece, 0)
            made[0] = until

    def one_slot(s):
        parts = [0] + [1 + s * per_slot + k for k in range(per_slot)]
        for i in parts:
            last(i // chunk)
        total = None
        for a in range(0, len(parts), 2):
            pieces = [
                held[:, i // chunk, i % chunk].reshape(lev_count * block, 128) for i in parts[a : a + 2]
            ]
            lhs = jnp.concatenate(pieces, axis=1)
            term = jnp.dot(lhs, rhs[s, a * 128 : (a + 2) * 128], preferred_element_type=jnp.float32)
            total = term if total is None else total + term
        groups = total.reshape(wav_count, total.shape[0] // wav_count, 256)
        both = jnp.concatenate([groups[:, :, :128], groups[:, :, 128:]], axis=1)
        ready[s] = both.astype(jnp.bfloat16)

        place = early.at[s, w] if s < EARLY else late_ref.at[s - EARLY, w]

        def send(k, _):
            peer = lax.rem(w + k, wav_count)
            pltpu.make_async_remote_copy(
                src_ref=ready.at[s, peer],
                dst_ref=place,
                send_sem=out_send,
                recv_sem=out_recv.at[s],
                device_id={"wav": peer},
                device_id_type=MESH,
            ).start()
            return 0

        lax.fori_loop(1, wav_count, send, 0)
        if s < EARLY:
            early[s, w] = ready[s, w]
        else:
            late_ref[s - EARLY, w] = ready[s, w]

    for entry in order:
        kind, value = entry[0], entry[1:]
        if kind == "hop":
            step(*value)
        elif kind == "slot":
            one_slot(*value)
        elif kind == "basis":
            more_basis(*value)
        elif kind == "mask":
            loads[1].wait()
            loads[4].wait()
            for s in range(slots):
                mask_slot(s)
        else:
            loads[2].wait()
            loads[3].wait()
            start_basis()
    more_basis(rows * strips)
    for c in range(chunks):
        last(c)

    def arrival(s):
        target = early.at[s, 1:] if s < EARLY else late_ref.at[s - EARLY, 1:]
        pltpu.make_async_copy(target, target, out_recv.at[s]).wait()

    for s in range(EARLY):
        arrival(s)
    both = early.shape[2]
    for s in range(EARLY):
        unpack(flat.at[pl.ds(s * wav_count * PITCH, wav_count * PITCH)], early.at[s].reshape(wav_count * both, 128), wav_count, both)

    turned[...] = jnp.zeros_like(turned)

    def one_row(r, _):
        lon = longitudes(lat_ref[w * rows + r])
        turn_row(waves, rows, 64, sums.shape[1] // 64, EARLY * wav_count, lanes[:, :128], flat, r, lon, turned)
        sums[r] = multiply(turned, [table[0, r, c] for c in range(WIDTH // 128)])
        return 0

    lax.fori_loop(0, rows, one_row, 0)

    for side in (0, 1):
        for d in range(half):
            for c in range(chunks):
                if goes(side, d, c):
                    hop(side, d, c).wait_send()

    pltpu.make_async_copy(ready.at[:, 1:], ready.at[:, 1:], out_send).wait()
    for s in range(EARLY, slots):
        arrival(s)


def plan(slots):
    hops = [(0, c) for c in (0, 1, 2, 3, 8, 5, 10, 4, 6, 9)]
    order = [("hop", *hop) for hop in hops]
    order += [("mask",), ("start",), ("basis", 24)]
    later = [(1, 0), (1, 1), (1, 2), (0, 7), (1, 3), (1, 5), (1, 8), (1, 4), (1, 6), (1, 9), (2, 0), (2, 1)]
    later += [(1, 10), (2, 2), (2, 3), (2, 5), (1, 7), (2, 4), (2, 6), (3, 0), (2, 8), (3, 1), (2, 10), (3, 2)]
    later += [(2, 9), (3, 4), (3, 3), (3, 8), (3, 6), (2, 7), (3, 5)]
    for i, hop in enumerate(later):
        order.append(("hop", *hop))
        if i % 3 == 2:
            order.append(("basis", 4))
    order += [("slot", 0), ("hop", 3, 10), ("slot", 1), ("hop", 3, 7), ("hop", 3, 9)]
    return order + [("slot", s) for s in range(2, slots)]


def exchange(spectral, legendre, wave_pair, lat_slot):
    slots, fold, _ = spectral.shape
    wav_count = lax.axis_size("wav")
    lev_count = lax.axis_size("lev")
    block = legendre.shape[2]
    rows = block * lev_count // wav_count
    total = wave_pair.shape[0]
    turned = jnp.swapaxes(legendre, 1, 2)
    tiles = 1 + slots * (fold // 128)
    chunk = 2
    chunks = tiles // chunk
    half = lev_count // 2
    moved = (2 * NLAT + 16 + WIDTH - 1) // WIDTH * 64
    return pl.pallas_call(
        functools.partial(exchange_kernel, fold - 1, slots, fold, plan(slots)),
        out_shape=[
            jax.ShapeDtypeStruct((slots - EARLY, wav_count, 2 * rows, 128), jnp.bfloat16),
            jax.ShapeDtypeStruct((2, rows, WIDTH // 128, 512, 128), jnp.bfloat16),
            jax.ShapeDtypeStruct((rows, moved, WIDTH), jnp.float32),
        ],
        in_specs=[pl.BlockSpec(memory_space=pl.ANY)] * 5,
        out_specs=[pl.BlockSpec(memory_space=pltpu.VMEM)] * 3,
        scratch_shapes=[
            pltpu.SMEM(wave_pair.shape, jnp.int32),
            pltpu.VMEM((1, total), jnp.int32),
            pltpu.SMEM(lat_slot.shape, jnp.int32),
            pltpu.VMEM(turned.shape, jnp.bfloat16),
            pltpu.VMEM(spectral.shape, jnp.bfloat16),
            pltpu.VMEM((lev_count, chunks, chunk, block, 128), jnp.bfloat16),
            pltpu.VMEM((slots, 512, 256), jnp.bfloat16),
            pltpu.VMEM((slots, wav_count, 2 * rows, 128), jnp.bfloat16),
            pltpu.VMEM((256, 128), jnp.float32),
            pltpu.VMEM((8, 256), jnp.float32),
            pltpu.VMEM((EARLY, wav_count, 2 * rows, 128), jnp.bfloat16),
            pltpu.VMEM((EARLY * wav_count * PITCH, 128), jnp.float32),
            pltpu.VMEM((4, moved, 128), jnp.bfloat16),
            pltpu.SemaphoreType.DMA((5,)),
            pltpu.SemaphoreType.DMA((2, half, chunks)),
            pltpu.SemaphoreType.DMA((2, half, chunks)),
            pltpu.SemaphoreType.DMA,
            pltpu.SemaphoreType.DMA((slots,)),
        ],
        compiler_params=pltpu.CompilerParams(
            collective_id=0, has_side_effects=True, vmem_limit_bytes=GRANT
        ),
        name="exchange",
    )(*(pltpu.with_memory_space_constraint(x, pltpu.HBM) for x in (wave_pair, wave_pair.reshape(1, total), lat_slot, turned, spectral)))


def synthesis_kernel(waves, rows, together, slots, pair_ref, lat_ref, in_ref, table, sums, out_ref, flat, lanes, *turned):
    step = pl.program_id(0)
    layers = out_ref.shape[1]
    width = out_ref.shape[2]
    blocks = (width + WIDTH - 1) // WIDTH
    count = in_ref.shape[0] // (2 * rows)

    @pl.when(step == 0)
    def _():
        unpack(flat, in_ref, count, 2 * rows)
        lanes[...] = lined_up(pair_ref[...].astype(jnp.float32), EARLY, slots, lax.axis_size("wav"), slots)
        for buffer in turned:
            buffer[...] = jnp.zeros_like(buffer)

    lengths = []
    for i in range(together):
        r = step * together + i
        lengths.append(longitudes(lat_ref[lax.axis_index("wav") * rows + r]))
        turn_row(waves, rows, layers, blocks, count, lanes[...], flat, r, lengths[i], turned[i])

    for i in range(together):
        result = sums[i] + multiply(turned[i], [table[0, i, c] for c in range(WIDTH // 128)])
        for b in range(blocks):
            size = min(WIDTH, width - b * WIDTH)
            col = lax.broadcasted_iota(jnp.int32, (layers, size), 1) + b * WIDTH
            piece = result[b * layers : (b + 1) * layers, :size]
            piece = jnp.where(col < lengths[i], piece, 0.0).astype(jnp.bfloat16)
            out_ref[i, :, b * WIDTH : b * WIDTH + size] = piece


def synthesis(late, table, sums, wave_pair, lat_slot, slots, waves):
    held, wav_count, both, _ = late.shape
    rows = both // 2
    total = wave_pair.shape[0]
    layers = 64
    width = 2 * NLAT + 16
    together = 2
    flat = late.reshape(held * wav_count * both, 128)
    return pl.pallas_call(
        functools.partial(synthesis_kernel, waves, rows, together, slots),
        grid=(rows // together,),
        out_shape=jax.ShapeDtypeStruct((rows, layers, width), jnp.bfloat16),
        in_specs=[
            pl.BlockSpec((1, total), lambda r: (0, 0)),
            pl.BlockSpec(memory_space=pltpu.SMEM),
            pl.BlockSpec(flat.shape, lambda r: (0, 0)),
            pl.BlockSpec((1, together, *table.shape[2:]), lambda r: (1, r, 0, 0, 0)),
            pl.BlockSpec((together, *sums.shape[1:]), lambda r: (r, 0, 0)),
        ],
        out_specs=pl.BlockSpec((together, layers, width), lambda r: (r, 0, 0)),
        scratch_shapes=[
            pltpu.VMEM((held * wav_count * PITCH, 128), jnp.float32),
            pltpu.VMEM((8, 128), jnp.float32),
        ]
        + [pltpu.VMEM((4, sums.shape[1], 128), jnp.bfloat16)] * together,
        compiler_params=pltpu.CompilerParams(
            dimension_semantics=("arbitrary",), vmem_limit_bytes=GRANT
        ),
        name="synthesis",
    )(
        pltpu.with_memory_space_constraint(wave_pair.reshape(1, total), pltpu.HBM),
        pltpu.with_memory_space_constraint(lat_slot, pltpu.HBM),
        flat,
        table,
        sums,
    )


def on_device(spectral, legendre, wave_pair, lat_slot):
    late, table, sums = exchange(spectral, legendre, wave_pair, lat_slot)
    slots, fold, _ = spectral.shape
    return synthesis(late, table, sums, wave_pair, lat_slot, slots, fold - 1)


def solution(mesh):
    return jax.shard_map(
        on_device,
        mesh=mesh,
        in_specs=(P("wav", None, "lev"), P("wav", None, "lev"), P(), P()),
        out_specs=P("wav", "lev", None),
        check_vma=False,
    )
```

```python
import functools

import jax
import jax.numpy as jnp
import numpy as np
from jax import lax
from jax.experimental import pallas as pl
from jax.experimental.pallas import tpu as pltpu
from jax.sharding import PartitionSpec as P

NLAT = 800
WIDTH = 256
PITCH = 24
EARLY = 3
GRANT = 20 * 2**20
MESH = pl.DeviceIdType.MESH


def poly_in_square(fn, degree):
    nodes = np.cos(np.pi * (np.arange(200) + 0.5) / 200)
    top = 0.52**2
    z = (nodes + 1) * 0.5 * top
    fit = np.polynomial.chebyshev.Chebyshev.fit(z, fn(np.sqrt(z)), degree, domain=[0, top])
    return [float(c) for c in fit.convert(kind=np.polynomial.Polynomial).coef]


SIN_COEF = poly_in_square(lambda x: np.sin(np.pi * x) / x, 5)
COS_COEF = poly_in_square(lambda x: np.cos(np.pi * x), 5)


def horner(coef, z):
    acc = jnp.full_like(z, coef[-1])
    for c in coef[-2::-1]:
        acc = acc * z + c
    return acc


def half_angle(steps, count, inverse):
    turns = jnp.floor(steps * inverse + 0.5)
    x = (steps - turns * count) * inverse
    z = x * x
    return x * horner(SIN_COEF, z), horner(COS_COEF, z)


def lined_up(pairs, first, past, wav_count, slots):
    lanes = 4 * wav_count
    index = lax.broadcasted_iota(jnp.int32, (pairs.shape[1], lanes), 0)
    lane = lax.broadcasted_iota(jnp.int32, (pairs.shape[1], lanes), 1)
    local = first + lax.div(lane, wav_count)
    chosen = (index == lax.rem(lane, wav_count) * slots + local) & (local < past)
    shifted = jnp.broadcast_to(pairs + 1.0, (16, pairs.shape[1])).astype(jnp.bfloat16)
    return jnp.dot(shifted, chosen.astype(jnp.bfloat16), preferred_element_type=jnp.float32)[:8] - 1.0


def unpack(flat, source, count, both):
    def piece(i, _):
        values = source[pl.ds(pl.multiple_of(i * both, both), both), :]
        flat[pl.ds(pl.multiple_of(i * PITCH, 8), both), :] = values.astype(jnp.float32)
        return 0

    lax.fori_loop(0, count, piece, 0, unroll=16)


def turn_row(waves, rows, layers, blocks, count, pairs, flat, r, points, turned):
    target = lax.broadcasted_iota(jnp.int32, (128, 128), 0)
    source = lax.broadcasted_iota(jnp.int32, (128, 128), 1)
    part = (target >= layers).astype(jnp.int32)
    place = (source == 2 * (target - part * layers) + part).astype(jnp.bfloat16)
    shift = lax.broadcasted_iota(jnp.int32, (8, count), 0).astype(jnp.float32) * WIDTH
    inverse = 1.0 / points
    for h in range(2):
        values = flat[pl.ds(h * rows + r, count, stride=PITCH), :].astype(jnp.bfloat16)
        split = lax.dot_general(place, values, (((1,), (1,)), ((), ())), preferred_element_type=jnp.float32)
        real, imag = split[:layers], split[layers:]
        m = pairs[:, :count] if h == 0 else (waves - 1.0) - pairs[:, :count]
        sin_half, cos_half = half_angle(m * shift, points, inverse)
        sines = 2.0 * sin_half * cos_half
        cosines = 1.0 - 2.0 * sin_half * sin_half
        for b in range(blocks):
            at = pl.ds(b * layers, layers)
            if b == 0:
                turned_real, turned_imag = real, imag
            else:
                cos_b, sin_b = cosines[b : b + 1], sines[b : b + 1]
                turned_real = real * cos_b - imag * sin_b
                turned_imag = real * sin_b + imag * cos_b
            turned[h, at, :count] = turned_real.astype(jnp.bfloat16)
            turned[2 + h, at, :count] = turned_imag.astype(jnp.bfloat16)


def multiply(turned, columns):
    lhs = jnp.concatenate([turned[k] for k in range(4)], axis=1)
    return jnp.dot(lhs, jnp.concatenate(columns, axis=1), preferred_element_type=jnp.float32)


def longitudes(latitude):
    return 20 + 4 * jnp.minimum(latitude, NLAT - 1 - latitude)


def exchange_kernel(
    waves,
    slots,
    fold,
    order,
    pair_hbm,
    pairs_hbm,
    lat_hbm,
    leg_hbm,
    spec_hbm,
    late_ref,
    table,
    sums,
    lanes,
    lengths,
    pair_ref,
    pairs_ref,
    lat_ref,
    leg_ref,
    spec_ref,
    held,
    rhs,
    ready,
    column,
    early,
    flat,
    turned,
    load_sem,
    send_sem,
    recv_sem,
    out_send,
    out_recv,
):
    wav_count = lax.axis_size("wav")
    lev_count = lax.axis_size("lev")
    w = lax.axis_index("wav")
    z = lax.axis_index("lev")
    right = lax.rem(z + 1, lev_count)
    left = lax.rem(z + lev_count - 1, lev_count)
    block = leg_ref.shape[1]
    full = (fold // 128) * 128
    rest = fold - full
    per_slot = full // 128
    chunks = held.shape[1]
    chunk = held.shape[2]
    rows = table.shape[1]
    total_slots = column.shape[0]

    sources = ((leg_hbm, leg_ref), (pair_hbm, pair_ref), (pairs_hbm, pairs_ref), (lat_hbm, lat_ref), (spec_hbm, spec_ref))
    loads = [pltpu.make_async_copy(src, dst, load_sem.at[i]) for i, (src, dst) in enumerate(sources)]
    for load in loads:
        load.start()

    barrier = pltpu.get_barrier_semaphore()
    for peer in (left, right):
        pl.semaphore_signal(barrier, inc=1, device_id={"lev": peer}, device_id_type=MESH)

    def greet(k, _):
        peer = lax.rem(w + k, wav_count)
        pl.semaphore_signal(barrier, inc=1, device_id={"wav": peer}, device_id_type=MESH)
        return 0

    lax.fori_loop(1, wav_count, greet, 0)

    loads[0].wait()
    tail = jnp.zeros((block, 128), jnp.float32)
    for s in range(slots):
        at_row = lax.broadcasted_iota(jnp.int32, (rest, 128), 0)
        at_col = lax.broadcasted_iota(jnp.int32, (rest, 128), 1)
        place = (at_col == at_row + rest * s).astype(jnp.bfloat16)
        tail += jnp.dot(leg_ref[s, :, full:fold], place, preferred_element_type=jnp.float32)
    held[z, 0, 0] = tail.astype(jnp.bfloat16)
    for s in range(slots):
        for k in range(per_slot):
            i = 1 + s * per_slot + k
            held[z, i // chunk, i % chunk] = leg_ref[s, :, k * 128 : (k + 1) * 128]

    pl.semaphore_wait(barrier, 2 + wav_count - 1)

    half = lev_count // 2

    def goes(side, d, c):
        return d < half - 1 or c % 2 == side

    def hop(side, d, c):
        owner = lax.rem(z + (lev_count - d if side == 0 else d), lev_count)
        return pltpu.make_async_remote_copy(
            src_ref=held.at[owner, c],
            dst_ref=held.at[owner, c],
            send_sem=send_sem.at[side, d, c],
            recv_sem=recv_sem.at[side, d, c],
            device_id={"lev": right if side == 0 else left},
            device_id_type=MESH,
        )

    def arrived(side, d, c):
        owner = lax.rem(z + (lev_count - d - 1 if side == 0 else d + 1), lev_count)
        pltpu.make_async_remote_copy(
            src_ref=held.at[owner, c],
            dst_ref=held.at[owner, c],
            send_sem=send_sem.at[side, d, c],
            recv_sem=recv_sem.at[side, d, c],
            device_id={"lev": right if side == 0 else left},
            device_id_type=MESH,
        ).wait_recv()

    def step(d, c):
        for side in (0, 1):
            if d:
                arrived(side, d - 1, c)
            if goes(side, d, c):
                hop(side, d, c).start()

    landed = set()

    def last(c):
        if c not in landed:
            landed.add(c)
            arrived(c % 2, half - 1, c)

    def mask_slot(s):
        border = (fold - 1) - pair_ref[w * slots + s]
        at_row = lax.broadcasted_iota(jnp.int32, (128, rest), 0)
        at_col = lax.broadcasted_iota(jnp.int32, (128, rest), 1)
        place = (at_row == at_col + rest * s).astype(jnp.bfloat16)
        row = lax.broadcasted_iota(jnp.int32, (128, 128), 0)
        ending = jnp.dot(place, spec_ref[s, full:fold, :], preferred_element_type=jnp.float32)
        below = row - rest * s + full < border
        rhs[s, 0:128, 0:128] = jnp.where(below, ending, 0.0).astype(jnp.bfloat16)
        rhs[s, 0:128, 128:256] = jnp.where(below, 0.0, ending).astype(jnp.bfloat16)
        for k in range(per_slot):
            piece = spec_ref[s, k * 128 : (k + 1) * 128, :].astype(jnp.float32)
            below = row + k * 128 < border
            at = (k + 1) * 128
            rhs[s, at : at + 128, 0:128] = jnp.where(below, piece, 0.0).astype(jnp.bfloat16)
            rhs[s, at : at + 128, 128:256] = jnp.where(below, 0.0, piece).astype(jnp.bfloat16)

    def start_basis():
        pairs = pairs_ref[...].astype(jnp.float32)
        for g in range(2):
            lined = lined_up(pairs, EARLY * g, slots if g else EARLY, wav_count, slots)
            lanes[:, g * 128 : (g + 1) * 128] = lined
            column[g * 128 : (g + 1) * 128, :] = jnp.transpose(jnp.broadcast_to(lined[:1], (128, 128)))

    strip = 32
    strips = total_slots // strip

    def basis_piece(i, _):
        r = lax.div(i, strips)
        block_of = lax.rem(i, strips)
        first = pl.multiple_of(block_of * strip, strip)
        group = lax.div(block_of, 4)
        local = pl.multiple_of(lax.rem(block_of, 4) * strip, strip)
        lon = longitudes(lat_ref[w * rows + r])
        highest = jnp.minimum(waves - 1, lax.shift_right_arithmetic(lon - 1, 1)).astype(jnp.float32)
        count = jnp.full((strip, 128), lon.astype(jnp.float32), jnp.float32)
        inverse = 1.0 / count
        lane = lax.broadcasted_iota(jnp.int32, (strip, 128), 1).astype(jnp.float32)
        pair = column[pl.ds(first, strip), :]
        for h in range(2):
            m = pair if h == 0 else (waves - 1.0) - pair
            weight = jnp.where(m == 0.0, 1.0, 2.0)
            weight = jnp.where((pair >= 0.0) & (m <= highest), weight, 0.0)
            minus = -2.0 * weight
            for c in range(WIDTH // 128):
                sin_half, cos_half = half_angle(m * (lane + 128.0 * c), count, inverse)
                scaled = sin_half * minus
                cos_part = (weight + scaled * sin_half).astype(jnp.bfloat16)
                sin_part = (scaled * cos_half).astype(jnp.bfloat16)
                table[group, r, c, pl.ds(h * 128 + local, strip), :] = cos_part
                table[group, r, c, pl.ds(256 + h * 128 + local, strip), :] = sin_part
        return 0

    made = [0]

    def more_basis(n):
        until = min(made[0] + n, rows * strips)
        if until > made[0]:
            lax.fori_loop(made[0], until, basis_piece, 0)
            made[0] = until

    def one_slot(s):
        parts = [0] + [1 + s * per_slot + k for k in range(per_slot)]
        for i in parts:
            last(i // chunk)
        total = None
        for a in range(0, len(parts), 2):
            pieces = [
                held[:, i // chunk, i % chunk].reshape(lev_count * block, 128) for i in parts[a : a + 2]
            ]
            lhs = jnp.concatenate(pieces, axis=1)
            term = jnp.dot(lhs, rhs[s, a * 128 : (a + 2) * 128], preferred_element_type=jnp.float32)
            total = term if total is None else total + term
        groups = total.reshape(wav_count, total.shape[0] // wav_count, 256)
        both = jnp.concatenate([groups[:, :, :128], groups[:, :, 128:]], axis=1)
        ready[s] = both.astype(jnp.bfloat16)

        place = early.at[s, w] if s < EARLY else late_ref.at[s - EARLY, w]

        def send(k, _):
            peer = lax.rem(w + k, wav_count)
            pltpu.make_async_remote_copy(
                src_ref=ready.at[s, peer],
                dst_ref=place,
                send_sem=out_send,
                recv_sem=out_recv.at[s],
                device_id={"wav": peer},
                device_id_type=MESH,
            ).start()
            return 0

        lax.fori_loop(1, wav_count, send, 0)
        if s < EARLY:
            early[s, w] = ready[s, w]
        else:
            late_ref[s - EARLY, w] = ready[s, w]

    for entry in order:
        kind, value = entry[0], entry[1:]
        if kind == "hop":
            step(*value)
        elif kind == "slot":
            one_slot(*value)
        elif kind == "basis":
            more_basis(*value)
        elif kind == "mask":
            loads[1].wait()
            loads[4].wait()
            for s in range(slots):
                mask_slot(s)
        else:
            loads[2].wait()
            loads[3].wait()
            start_basis()
    more_basis(rows * strips)
    for c in range(chunks):
        last(c)

    def arrival(s):
        target = early.at[s, 1:] if s < EARLY else late_ref.at[s - EARLY, 1:]
        pltpu.make_async_copy(target, target, out_recv.at[s]).wait()

    for s in range(EARLY):
        arrival(s)
    both = early.shape[2]
    for s in range(EARLY):
        unpack(flat.at[pl.ds(s * wav_count * PITCH, wav_count * PITCH)], early.at[s].reshape(wav_count * both, 128), wav_count, both)

    turned[...] = jnp.zeros_like(turned)

    def one_row(r, _):
        lengths[r] = jnp.full((8, 128), longitudes(lat_ref[w * rows + r]).astype(jnp.float32), jnp.float32)
        turn_row(waves, rows, 64, sums.shape[1] // 64, EARLY * wav_count, lanes[:, :128], flat, r, lengths[r][:, : EARLY * wav_count], turned)
        sums[r] = multiply(turned, [table[0, r, c] for c in range(WIDTH // 128)])
        return 0

    lax.fori_loop(0, rows, one_row, 0)

    for side in (0, 1):
        for d in range(half):
            for c in range(chunks):
                if goes(side, d, c):
                    hop(side, d, c).wait_send()

    pltpu.make_async_copy(ready.at[:, 1:], ready.at[:, 1:], out_send).wait()
    for s in range(EARLY, slots):
        arrival(s)


def plan(slots):
    hops = [(0, c) for c in (0, 1, 2, 3, 8, 5, 10, 4, 6, 9)]
    order = [("hop", *hop) for hop in hops]
    order += [("mask",), ("start",), ("basis", 24)]
    later = [(1, 0), (1, 1), (1, 2), (0, 7), (1, 3), (1, 5), (1, 8), (1, 4), (1, 6), (1, 9), (2, 0), (2, 1)]
    later += [(1, 10), (2, 2), (2, 3), (2, 5), (1, 7), (2, 4), (2, 6), (3, 0), (2, 8), (3, 1), (2, 10), (3, 2)]
    later += [(2, 9), (3, 4), (3, 3), (3, 8), (3, 6), (2, 7), (3, 5)]
    for i, hop in enumerate(later):
        order.append(("hop", *hop))
        if i % 3 == 2:
            order.append(("basis", 4))
    order += [("slot", 0), ("hop", 3, 10), ("slot", 1), ("hop", 3, 7), ("hop", 3, 9)]
    return order + [("slot", s) for s in range(2, slots)]


def exchange(spectral, legendre, wave_pair, lat_slot):
    slots, fold, _ = spectral.shape
    wav_count = lax.axis_size("wav")
    lev_count = lax.axis_size("lev")
    block = legendre.shape[2]
    rows = block * lev_count // wav_count
    total = wave_pair.shape[0]
    turned = jnp.swapaxes(legendre, 1, 2)
    tiles = 1 + slots * (fold // 128)
    chunk = 2
    chunks = tiles // chunk
    half = lev_count // 2
    moved = (2 * NLAT + 16 + WIDTH - 1) // WIDTH * 64
    return pl.pallas_call(
        functools.partial(exchange_kernel, fold - 1, slots, fold, plan(slots)),
        out_shape=[
            jax.ShapeDtypeStruct((slots - EARLY, wav_count, 2 * rows, 128), jnp.bfloat16),
            jax.ShapeDtypeStruct((2, rows, WIDTH // 128, 512, 128), jnp.bfloat16),
            jax.ShapeDtypeStruct((rows, moved, WIDTH), jnp.float32),
            jax.ShapeDtypeStruct((8, 256), jnp.float32),
            jax.ShapeDtypeStruct((rows, 8, 128), jnp.float32),
        ],
        in_specs=[pl.BlockSpec(memory_space=pl.ANY)] * 5,
        out_specs=[pl.BlockSpec(memory_space=pltpu.VMEM)] * 5,
        scratch_shapes=[
            pltpu.SMEM(wave_pair.shape, jnp.int32),
            pltpu.VMEM((1, total), jnp.int32),
            pltpu.SMEM(lat_slot.shape, jnp.int32),
            pltpu.VMEM(turned.shape, jnp.bfloat16),
            pltpu.VMEM(spectral.shape, jnp.bfloat16),
            pltpu.VMEM((lev_count, chunks, chunk, block, 128), jnp.bfloat16),
            pltpu.VMEM((slots, 512, 256), jnp.bfloat16),
            pltpu.VMEM((slots, wav_count, 2 * rows, 128), jnp.bfloat16),
            pltpu.VMEM((256, 128), jnp.float32),
            pltpu.VMEM((EARLY, wav_count, 2 * rows, 128), jnp.bfloat16),
            pltpu.VMEM((EARLY * wav_count * PITCH, 128), jnp.float32),
            pltpu.VMEM((4, moved, 128), jnp.bfloat16),
            pltpu.SemaphoreType.DMA((5,)),
            pltpu.SemaphoreType.DMA((2, half, chunks)),
            pltpu.SemaphoreType.DMA((2, half, chunks)),
            pltpu.SemaphoreType.DMA,
            pltpu.SemaphoreType.DMA((slots,)),
        ],
        compiler_params=pltpu.CompilerParams(
            collective_id=0, has_side_effects=True, vmem_limit_bytes=GRANT
        ),
        name="exchange",
    )(*(pltpu.with_memory_space_constraint(x, pltpu.HBM) for x in (wave_pair, wave_pair.reshape(1, total), lat_slot, turned, spectral)))


def synthesis_kernel(waves, together, in_ref, table, sums, lanes, lengths, out_ref, flat, *turned):
    step = pl.program_id(0)
    layers = out_ref.shape[1]
    width = out_ref.shape[2]
    blocks = (width + WIDTH - 1) // WIDTH
    count = flat.shape[0] // PITCH
    both = in_ref.shape[0] // count

    @pl.when(step == 0)
    def _():
        unpack(flat, in_ref, count, both)
        if count < 128:
            for buffer in turned:
                buffer[...] = jnp.zeros_like(buffer)

    for i in range(together):
        r = step * together + i
        turn_row(waves, both // 2, layers, blocks, count, lanes[:, 128:], flat, r, lengths[i][:, :count], turned[i])

    for i in range(together):
        result = sums[i] + multiply(turned[i], [table[0, i, c] for c in range(WIDTH // 128)])
        length = jnp.concatenate([lengths[i][:1]] * (WIDTH // 128), axis=1)
        for b in range(blocks):
            size = min(WIDTH, width - b * WIDTH)
            col = (lax.broadcasted_iota(jnp.int32, (layers, size), 1) + b * WIDTH).astype(jnp.float32)
            piece = result[b * layers : (b + 1) * layers, :size]
            piece = jnp.where(col < length[:, :size], piece, 0.0).astype(jnp.bfloat16)
            out_ref[i, :, b * WIDTH : b * WIDTH + size] = piece


def synthesis(late, table, sums, lanes, lengths, waves):
    held, wav_count, both, _ = late.shape
    rows = both // 2
    layers = 64
    width = 2 * NLAT + 16
    together = 2
    flat = late.reshape(held * wav_count * both, 128)
    return pl.pallas_call(
        functools.partial(synthesis_kernel, waves, together),
        grid=(rows // together,),
        out_shape=jax.ShapeDtypeStruct((rows, layers, width), jnp.bfloat16),
        in_specs=[
            pl.BlockSpec(flat.shape, lambda r: (0, 0)),
            pl.BlockSpec((1, together, *table.shape[2:]), lambda r: (1, r, 0, 0, 0)),
            pl.BlockSpec((together, *sums.shape[1:]), lambda r: (r, 0, 0)),
            pl.BlockSpec(lanes.shape, lambda r: (0, 0)),
            pl.BlockSpec((together, *lengths.shape[1:]), lambda r: (r, 0, 0)),
        ],
        out_specs=pl.BlockSpec((together, layers, width), lambda r: (r, 0, 0)),
        scratch_shapes=[
            pltpu.VMEM((held * wav_count * PITCH, 128), jnp.float32),
        ]
        + [pltpu.VMEM((4, sums.shape[1], 128), jnp.bfloat16)] * together,
        compiler_params=pltpu.CompilerParams(
            dimension_semantics=("arbitrary",), vmem_limit_bytes=GRANT
        ),
        name="synthesis",
    )(flat, table, sums, lanes, lengths)


def on_device(spectral, legendre, wave_pair, lat_slot):
    late, table, sums, lanes, lengths = exchange(spectral, legendre, wave_pair, lat_slot)
    return synthesis(late, table, sums, lanes, lengths, spectral.shape[1] - 1)


def solution(mesh):
    return jax.shard_map(
        on_device,
        mesh=mesh,
        in_specs=(P("wav", None, "lev"), P("wav", None, "lev"), P(), P()),
        out_specs=P("wav", "lev", None),
        check_vma=False,
    )
```

```python
import functools

import jax
import jax.numpy as jnp
import numpy as np
from jax import lax
from jax.experimental import pallas as pl
from jax.experimental.pallas import tpu as pltpu
from jax.sharding import PartitionSpec as P

NLAT = 800
WIDTH = 256
PITCH = 24
EARLY = 3
GRANT = 20 * 2**20
MESH = pl.DeviceIdType.MESH


def poly_in_square(fn, degree):
    nodes = np.cos(np.pi * (np.arange(200) + 0.5) / 200)
    top = 0.52**2
    z = (nodes + 1) * 0.5 * top
    fit = np.polynomial.chebyshev.Chebyshev.fit(z, fn(np.sqrt(z)), degree, domain=[0, top])
    return [float(c) for c in fit.convert(kind=np.polynomial.Polynomial).coef]


SIN_COEF = poly_in_square(lambda x: np.sin(np.pi * x) / x, 5)
COS_COEF = poly_in_square(lambda x: np.cos(np.pi * x), 5)


def horner(coef, z):
    acc = jnp.full_like(z, coef[-1])
    for c in coef[-2::-1]:
        acc = acc * z + c
    return acc


def half_angle(steps, count, inverse):
    turns = jnp.floor(steps * inverse + 0.5)
    x = (steps - turns * count) * inverse
    z = x * x
    return x * horner(SIN_COEF, z), horner(COS_COEF, z)


def lined_up(pairs, first, past, wav_count, slots):
    lanes = 4 * wav_count
    index = lax.broadcasted_iota(jnp.int32, (pairs.shape[1], lanes), 0)
    lane = lax.broadcasted_iota(jnp.int32, (pairs.shape[1], lanes), 1)
    local = first + lax.div(lane, wav_count)
    chosen = (index == lax.rem(lane, wav_count) * slots + local) & (local < past)
    shifted = jnp.broadcast_to(pairs + 1.0, (16, pairs.shape[1])).astype(jnp.bfloat16)
    return jnp.dot(shifted, chosen.astype(jnp.bfloat16), preferred_element_type=jnp.float32)[:8] - 1.0


def unpack(flat, source, count, both):
    def piece(i, _):
        values = source[pl.ds(pl.multiple_of(i * both, both), both), :]
        flat[pl.ds(pl.multiple_of(i * PITCH, 8), both), :] = values.astype(jnp.float32)
        return 0

    lax.fori_loop(0, count, piece, 0, unroll=16)


def turn_row(waves, rows, layers, blocks, count, pairs, flat, r, points, turned):
    target = lax.broadcasted_iota(jnp.int32, (128, 128), 0)
    source = lax.broadcasted_iota(jnp.int32, (128, 128), 1)
    part = (target >= layers).astype(jnp.int32)
    place = (source == 2 * (target - part * layers) + part).astype(jnp.bfloat16)
    shift = lax.broadcasted_iota(jnp.int32, (8, count), 0).astype(jnp.float32) * WIDTH
    inverse = 1.0 / points
    for h in range(2):
        values = flat[pl.ds(h * rows + r, count, stride=PITCH), :].astype(jnp.bfloat16)
        split = lax.dot_general(place, values, (((1,), (1,)), ((), ())), preferred_element_type=jnp.float32)
        real, imag = split[:layers], split[layers:]
        m = pairs[:, :count] if h == 0 else (waves - 1.0) - pairs[:, :count]
        sin_half, cos_half = half_angle(m * shift, points, inverse)
        sines = 2.0 * sin_half * cos_half
        cosines = 1.0 - 2.0 * sin_half * sin_half
        for b in range(blocks):
            at = pl.ds(b * layers, layers)
            if b == 0:
                turned_real, turned_imag = real, imag
            else:
                cos_b, sin_b = cosines[b : b + 1], sines[b : b + 1]
                turned_real = real * cos_b - imag * sin_b
                turned_imag = real * sin_b + imag * cos_b
            turned[h, at, :count] = turned_real.astype(jnp.bfloat16)
            turned[2 + h, at, :count] = turned_imag.astype(jnp.bfloat16)


def multiply(turned, columns):
    lhs = jnp.concatenate([turned[k] for k in range(4)], axis=1)
    return jnp.dot(lhs, jnp.concatenate(columns, axis=1), preferred_element_type=jnp.float32)


def longitudes(latitude):
    return 20 + 4 * jnp.minimum(latitude, NLAT - 1 - latitude)


def exchange_kernel(
    waves,
    slots,
    fold,
    order,
    pair_hbm,
    pairs_hbm,
    lat_hbm,
    leg_hbm,
    spec_hbm,
    late_ref,
    table,
    sums,
    lanes,
    lengths,
    pair_ref,
    pairs_ref,
    lat_ref,
    leg_ref,
    spec_ref,
    held,
    rhs,
    ready,
    column,
    early,
    flat,
    turned,
    load_sem,
    send_sem,
    recv_sem,
    out_send,
    out_recv,
):
    wav_count = lax.axis_size("wav")
    lev_count = lax.axis_size("lev")
    w = lax.axis_index("wav")
    z = lax.axis_index("lev")
    right = lax.rem(z + 1, lev_count)
    left = lax.rem(z + lev_count - 1, lev_count)
    block = leg_ref.shape[1]
    full = (fold // 128) * 128
    rest = fold - full
    per_slot = full // 128
    chunks = held.shape[1]
    chunk = held.shape[2]
    rows = table.shape[1]
    total_slots = column.shape[0]

    sources = ((leg_hbm, leg_ref), (pair_hbm, pair_ref), (pairs_hbm, pairs_ref), (lat_hbm, lat_ref), (spec_hbm, spec_ref))
    loads = [pltpu.make_async_copy(src, dst, load_sem.at[i]) for i, (src, dst) in enumerate(sources)]
    for load in loads:
        load.start()

    barrier = pltpu.get_barrier_semaphore()
    for peer in (left, right):
        pl.semaphore_signal(barrier, inc=1, device_id={"lev": peer}, device_id_type=MESH)

    def greet(k, _):
        peer = lax.rem(w + k, wav_count)
        pl.semaphore_signal(barrier, inc=1, device_id={"wav": peer}, device_id_type=MESH)
        return 0

    lax.fori_loop(1, wav_count, greet, 0)

    loads[0].wait()
    tail = jnp.zeros((block, 128), jnp.float32)
    for s in range(slots):
        at_row = lax.broadcasted_iota(jnp.int32, (rest, 128), 0)
        at_col = lax.broadcasted_iota(jnp.int32, (rest, 128), 1)
        place = (at_col == at_row + rest * s).astype(jnp.bfloat16)
        tail += jnp.dot(leg_ref[s, :, full:fold], place, preferred_element_type=jnp.float32)
    held[z, 0, 0] = tail.astype(jnp.bfloat16)
    for s in range(slots):
        for k in range(per_slot):
            i = 1 + s * per_slot + k
            held[z, i // chunk, i % chunk] = leg_ref[s, :, k * 128 : (k + 1) * 128]

    pl.semaphore_wait(barrier, 2 + wav_count - 1)

    half = lev_count // 2

    def goes(side, d, c):
        return d < half - 1 or c % 2 == side

    def hop(side, d, c):
        owner = lax.rem(z + (lev_count - d if side == 0 else d), lev_count)
        return pltpu.make_async_remote_copy(
            src_ref=held.at[owner, c],
            dst_ref=held.at[owner, c],
            send_sem=send_sem.at[side, d, c],
            recv_sem=recv_sem.at[side, d, c],
            device_id={"lev": right if side == 0 else left},
            device_id_type=MESH,
        )

    def arrived(side, d, c):
        owner = lax.rem(z + (lev_count - d - 1 if side == 0 else d + 1), lev_count)
        pltpu.make_async_remote_copy(
            src_ref=held.at[owner, c],
            dst_ref=held.at[owner, c],
            send_sem=send_sem.at[side, d, c],
            recv_sem=recv_sem.at[side, d, c],
            device_id={"lev": right if side == 0 else left},
            device_id_type=MESH,
        ).wait_recv()

    def step(d, c):
        for side in (0, 1):
            if d:
                arrived(side, d - 1, c)
            if goes(side, d, c):
                hop(side, d, c).start()

    landed = set()

    def last(c):
        if c not in landed:
            landed.add(c)
            arrived(c % 2, half - 1, c)

    def mask_slot(s):
        border = (fold - 1) - pair_ref[w * slots + s]
        at_row = lax.broadcasted_iota(jnp.int32, (128, rest), 0)
        at_col = lax.broadcasted_iota(jnp.int32, (128, rest), 1)
        place = (at_row == at_col + rest * s).astype(jnp.bfloat16)
        row = lax.broadcasted_iota(jnp.int32, (128, 128), 0)
        ending = jnp.dot(place, spec_ref[s, full:fold, :], preferred_element_type=jnp.float32)
        below = row - rest * s + full < border
        rhs[s, 0:128, 0:128] = jnp.where(below, ending, 0.0).astype(jnp.bfloat16)
        rhs[s, 0:128, 128:256] = jnp.where(below, 0.0, ending).astype(jnp.bfloat16)
        for k in range(per_slot):
            piece = spec_ref[s, k * 128 : (k + 1) * 128, :].astype(jnp.float32)
            below = row + k * 128 < border
            at = (k + 1) * 128
            rhs[s, at : at + 128, 0:128] = jnp.where(below, piece, 0.0).astype(jnp.bfloat16)
            rhs[s, at : at + 128, 128:256] = jnp.where(below, 0.0, piece).astype(jnp.bfloat16)

    def start_basis():
        pairs = pairs_ref[...].astype(jnp.float32)
        for g in range(2):
            lined = lined_up(pairs, EARLY * g, slots if g else EARLY, wav_count, slots)
            lanes[:, g * 128 : (g + 1) * 128] = lined
            column[g * 128 : (g + 1) * 128, :] = jnp.transpose(jnp.broadcast_to(lined[:1], (128, 128)))

    strip = 32
    strips = total_slots // strip

    def basis_piece(i, _):
        r = lax.div(i, strips)
        block_of = lax.rem(i, strips)
        first = pl.multiple_of(block_of * strip, strip)
        group = lax.div(block_of, 4)
        local = pl.multiple_of(lax.rem(block_of, 4) * strip, strip)
        lon = longitudes(lat_ref[w * rows + r])
        highest = jnp.minimum(waves - 1, lax.shift_right_arithmetic(lon - 1, 1)).astype(jnp.float32)
        count = jnp.full((strip, 128), lon.astype(jnp.float32), jnp.float32)
        inverse = 1.0 / count
        lane = lax.broadcasted_iota(jnp.int32, (strip, 128), 1).astype(jnp.float32)
        pair = column[pl.ds(first, strip), :]
        for h in range(2):
            m = pair if h == 0 else (waves - 1.0) - pair
            weight = jnp.where(m == 0.0, 1.0, 2.0)
            weight = jnp.where((pair >= 0.0) & (m <= highest), weight, 0.0)
            minus = -2.0 * weight
            for c in range(WIDTH // 128):
                sin_half, cos_half = half_angle(m * (lane + 128.0 * c), count, inverse)
                scaled = sin_half * minus
                cos_part = (weight + scaled * sin_half).astype(jnp.bfloat16)
                sin_part = (scaled * cos_half).astype(jnp.bfloat16)
                table[group, r, c, pl.ds(h * 128 + local, strip), :] = cos_part
                table[group, r, c, pl.ds(256 + h * 128 + local, strip), :] = sin_part
        return 0

    made = [0]

    def more_basis(n):
        until = min(made[0] + n, rows * strips)
        if until > made[0]:
            lax.fori_loop(made[0], until, basis_piece, 0)
            made[0] = until

    def one_slot(s):
        parts = [0] + [1 + s * per_slot + k for k in range(per_slot)]
        for i in parts:
            last(i // chunk)
        total = None
        for a in range(0, len(parts), 2):
            pieces = [
                held[:, i // chunk, i % chunk].reshape(lev_count * block, 128) for i in parts[a : a + 2]
            ]
            lhs = jnp.concatenate(pieces, axis=1)
            term = jnp.dot(lhs, rhs[s, a * 128 : (a + 2) * 128], preferred_element_type=jnp.float32)
            total = term if total is None else total + term
        groups = total.reshape(wav_count, total.shape[0] // wav_count, 256)
        both = jnp.concatenate([groups[:, :, :128], groups[:, :, 128:]], axis=1)
        ready[s] = both.astype(jnp.bfloat16)

        place = early.at[s, w] if s < EARLY else late_ref.at[s - EARLY, w]

        def send(k, _):
            peer = lax.rem(w + k, wav_count)
            pltpu.make_async_remote_copy(
                src_ref=ready.at[s, peer],
                dst_ref=place,
                send_sem=out_send,
                recv_sem=out_recv.at[s],
                device_id={"wav": peer},
                device_id_type=MESH,
            ).start()
            return 0

        lax.fori_loop(1, wav_count, send, 0)
        if s < EARLY:
            early[s, w] = ready[s, w]
        else:
            late_ref[s - EARLY, w] = ready[s, w]

    for entry in order:
        kind, value = entry[0], entry[1:]
        if kind == "hop":
            step(*value)
        elif kind == "slot":
            one_slot(*value)
        elif kind == "basis":
            more_basis(*value)
        elif kind == "mask":
            loads[1].wait()
            loads[4].wait()
            for s in range(slots):
                mask_slot(s)
        else:
            loads[2].wait()
            loads[3].wait()
            start_basis()
    more_basis(rows * strips)
    for c in range(chunks):
        last(c)

    def arrival(s):
        target = early.at[s, 1:] if s < EARLY else late_ref.at[s - EARLY, 1:]
        pltpu.make_async_copy(target, target, out_recv.at[s]).wait()

    for s in range(EARLY):
        arrival(s)
    both = early.shape[2]
    for s in range(EARLY):
        unpack(flat.at[pl.ds(s * wav_count * PITCH, wav_count * PITCH)], early.at[s].reshape(wav_count * both, 128), wav_count, both)

    turned[...] = jnp.zeros_like(turned)

    def one_row(r, _):
        lengths[r] = jnp.full((8, 128), longitudes(lat_ref[w * rows + r]).astype(jnp.float32), jnp.float32)
        turn_row(waves, rows, 64, sums.shape[1] // 64, EARLY * wav_count, lanes[:, :128], flat, r, lengths[r][:, : EARLY * wav_count], turned)
        sums[r] = multiply(turned, [table[0, r, c] for c in range(WIDTH // 128)])
        return 0

    lax.fori_loop(0, rows, one_row, 0)

    for side in (0, 1):
        for d in range(half):
            for c in range(chunks):
                if goes(side, d, c):
                    hop(side, d, c).wait_send()

    pltpu.make_async_copy(ready.at[:, 1:], ready.at[:, 1:], out_send).wait()
    for s in range(EARLY, slots):
        arrival(s)


def plan(slots):
    hops = [(0, c) for c in (0, 1, 2, 3, 8, 5, 10, 4, 6, 9)]
    order = [("hop", *hop) for hop in hops]
    order += [("mask",), ("start",), ("basis", 24)]
    later = [(1, 0), (1, 1), (1, 2), (0, 7), (1, 3), (1, 5), (1, 8), (1, 4), (1, 6), (1, 9), (2, 0), (2, 1)]
    later += [(1, 10), (2, 2), (2, 3), (2, 5), (1, 7), (2, 4), (2, 6), (3, 0), (2, 8), (3, 1), (2, 10), (3, 2)]
    later += [(2, 9), (3, 4), (3, 3), (3, 8), (3, 6), (2, 7), (3, 5)]
    for i, hop in enumerate(later):
        order.append(("hop", *hop))
        if i % 3 == 2:
            order.append(("basis", 4))
    order += [("slot", 0), ("hop", 3, 10), ("slot", 1), ("hop", 3, 7), ("hop", 3, 9)]
    return order + [("slot", s) for s in range(2, slots)]


def exchange(spectral, legendre, wave_pair, lat_slot):
    slots, fold, _ = spectral.shape
    wav_count = lax.axis_size("wav")
    lev_count = lax.axis_size("lev")
    block = legendre.shape[2]
    rows = block * lev_count // wav_count
    total = wave_pair.shape[0]
    turned = jnp.swapaxes(legendre, 1, 2)
    tiles = 1 + slots * (fold // 128)
    chunk = 2
    chunks = tiles // chunk
    half = lev_count // 2
    moved = (2 * NLAT + 16 + WIDTH - 1) // WIDTH * 64
    return pl.pallas_call(
        functools.partial(exchange_kernel, fold - 1, slots, fold, plan(slots)),
        out_shape=[
            jax.ShapeDtypeStruct((slots - EARLY, wav_count, 2 * rows, 128), jnp.bfloat16),
            jax.ShapeDtypeStruct((2, rows, WIDTH // 128, 512, 128), jnp.bfloat16),
            jax.ShapeDtypeStruct((rows, moved, WIDTH), jnp.float32),
            jax.ShapeDtypeStruct((8, 256), jnp.float32),
            jax.ShapeDtypeStruct((rows, 8, 128), jnp.float32),
        ],
        in_specs=[pl.BlockSpec(memory_space=pl.ANY)] * 5,
        out_specs=[pl.BlockSpec(memory_space=pltpu.VMEM)] * 5,
        scratch_shapes=[
            pltpu.SMEM(wave_pair.shape, jnp.int32),
            pltpu.VMEM((1, total), jnp.int32),
            pltpu.SMEM(lat_slot.shape, jnp.int32),
            pltpu.VMEM(turned.shape, jnp.bfloat16),
            pltpu.VMEM(spectral.shape, jnp.bfloat16),
            pltpu.VMEM((lev_count, chunks, chunk, block, 128), jnp.bfloat16),
            pltpu.VMEM((slots, 512, 256), jnp.bfloat16),
            pltpu.VMEM((slots, wav_count, 2 * rows, 128), jnp.bfloat16),
            pltpu.VMEM((256, 128), jnp.float32),
            pltpu.VMEM((EARLY, wav_count, 2 * rows, 128), jnp.bfloat16),
            pltpu.VMEM((EARLY * wav_count * PITCH, 128), jnp.float32),
            pltpu.VMEM((4, moved, 128), jnp.bfloat16),
            pltpu.SemaphoreType.DMA((5,)),
            pltpu.SemaphoreType.DMA((2, half, chunks)),
            pltpu.SemaphoreType.DMA((2, half, chunks)),
            pltpu.SemaphoreType.DMA,
            pltpu.SemaphoreType.DMA((slots,)),
        ],
        compiler_params=pltpu.CompilerParams(
            collective_id=0, has_side_effects=True, vmem_limit_bytes=GRANT
        ),
        name="exchange",
    )(*(pltpu.with_memory_space_constraint(x, pltpu.HBM) for x in (wave_pair, wave_pair.reshape(1, total), lat_slot, turned, spectral)))


def synthesis_kernel(waves, together, in_ref, table, sums, lanes, lengths, out_ref, flat, *turned):
    step = pl.program_id(0)
    layers = out_ref.shape[1]
    width = out_ref.shape[2]
    blocks = (width + WIDTH - 1) // WIDTH
    count = flat.shape[0] // PITCH
    both = in_ref.shape[0] // count

    @pl.when(step == 0)
    def _():
        unpack(flat, in_ref, count, both)
        if count < 128:
            for buffer in turned:
                buffer[...] = jnp.zeros_like(buffer)

    for i in range(together):
        r = step * together + i
        turn_row(waves, both // 2, layers, blocks, count, lanes[:, 128:], flat, r, lengths[i][:, :count], turned[i])

    for i in range(together):
        result = sums[i] + multiply(turned[i], [table[0, i, c] for c in range(WIDTH // 128)])
        length = jnp.concatenate([lengths[i][:1]] * (WIDTH // 128), axis=1)
        for b in range(blocks):
            size = min(WIDTH, width - b * WIDTH)
            col = (lax.broadcasted_iota(jnp.int32, (layers, size), 1) + b * WIDTH).astype(jnp.float32)
            piece = result[b * layers : (b + 1) * layers, :size]
            piece = jnp.where(col < length[:, :size], piece, 0.0).astype(jnp.bfloat16)
            out_ref[i, :, b * WIDTH : b * WIDTH + size] = piece


def synthesis(late, table, sums, lanes, lengths, waves):
    held, wav_count, both, _ = late.shape
    rows = both // 2
    layers = 64
    width = 2 * NLAT + 16
    together = 4
    flat = late.reshape(held * wav_count * both, 128)
    return pl.pallas_call(
        functools.partial(synthesis_kernel, waves, together),
        grid=(rows // together,),
        out_shape=jax.ShapeDtypeStruct((rows, layers, width), jnp.bfloat16),
        in_specs=[
            pl.BlockSpec(flat.shape, lambda r: (0, 0)),
            pl.BlockSpec((1, together, *table.shape[2:]), lambda r: (1, r, 0, 0, 0)),
            pl.BlockSpec((together, *sums.shape[1:]), lambda r: (r, 0, 0)),
            pl.BlockSpec(lanes.shape, lambda r: (0, 0)),
            pl.BlockSpec((together, *lengths.shape[1:]), lambda r: (r, 0, 0)),
        ],
        out_specs=pl.BlockSpec((together, layers, width), lambda r: (r, 0, 0)),
        scratch_shapes=[
            pltpu.VMEM((held * wav_count * PITCH, 128), jnp.float32),
        ]
        + [pltpu.VMEM((4, sums.shape[1], 128), jnp.bfloat16)] * together,
        compiler_params=pltpu.CompilerParams(
            dimension_semantics=("arbitrary",), vmem_limit_bytes=GRANT
        ),
        name="synthesis",
    )(flat, table, sums, lanes, lengths)


def on_device(spectral, legendre, wave_pair, lat_slot):
    late, table, sums, lanes, lengths = exchange(spectral, legendre, wave_pair, lat_slot)
    return synthesis(late, table, sums, lanes, lengths, spectral.shape[1] - 1)


def solution(mesh):
    return jax.shard_map(
        on_device,
        mesh=mesh,
        in_specs=(P("wav", None, "lev"), P("wav", None, "lev"), P(), P()),
        out_specs=P("wav", "lev", None),
        check_vma=False,
    )
```

```python
import functools

import jax
import jax.numpy as jnp
import numpy as np
from jax import lax
from jax.experimental import pallas as pl
from jax.experimental.pallas import tpu as pltpu
from jax.sharding import PartitionSpec as P

NLAT = 800
WIDTH = 256
PITCH = 24
EARLY = 3
GRANT = 20 * 2**20
MESH = pl.DeviceIdType.MESH


def poly_in_square(fn, degree):
    nodes = np.cos(np.pi * (np.arange(200) + 0.5) / 200)
    top = 0.52**2
    z = (nodes + 1) * 0.5 * top
    fit = np.polynomial.chebyshev.Chebyshev.fit(z, fn(np.sqrt(z)), degree, domain=[0, top])
    return [float(c) for c in fit.convert(kind=np.polynomial.Polynomial).coef]


SIN_COEF = poly_in_square(lambda x: np.sin(np.pi * x) / x, 5)
COS_COEF = poly_in_square(lambda x: np.cos(np.pi * x), 5)


def horner(coef, z):
    acc = jnp.full_like(z, coef[-1])
    for c in coef[-2::-1]:
        acc = acc * z + c
    return acc


def half_angle(steps, count, inverse):
    turns = jnp.floor(steps * inverse + 0.5)
    x = (steps - turns * count) * inverse
    z = x * x
    return x * horner(SIN_COEF, z), horner(COS_COEF, z)


def lined_up(pairs, first, past, wav_count, slots):
    lanes = 4 * wav_count
    index = lax.broadcasted_iota(jnp.int32, (pairs.shape[1], lanes), 0)
    lane = lax.broadcasted_iota(jnp.int32, (pairs.shape[1], lanes), 1)
    local = first + lax.div(lane, wav_count)
    chosen = (index == lax.rem(lane, wav_count) * slots + local) & (local < past)
    shifted = jnp.broadcast_to(pairs + 1.0, (16, pairs.shape[1])).astype(jnp.bfloat16)
    return jnp.dot(shifted, chosen.astype(jnp.bfloat16), preferred_element_type=jnp.float32)[:8] - 1.0


def unpack(flat, source, count, both):
    def piece(i, _):
        values = source[pl.ds(pl.multiple_of(i * both, both), both), :]
        flat[pl.ds(pl.multiple_of(i * PITCH, 8), both), :] = values.astype(jnp.float32)
        return 0

    lax.fori_loop(0, count, piece, 0, unroll=16)


def turn_row(waves, rows, layers, blocks, count, pairs, flat, r, points, turned):
    target = lax.broadcasted_iota(jnp.int32, (128, 128), 0)
    source = lax.broadcasted_iota(jnp.int32, (128, 128), 1)
    part = (target >= layers).astype(jnp.int32)
    place = (source == 2 * (target - part * layers) + part).astype(jnp.bfloat16)
    shift = lax.broadcasted_iota(jnp.int32, (8, count), 0).astype(jnp.float32) * WIDTH
    inverse = 1.0 / points
    for h in range(2):
        values = flat[pl.ds(h * rows + r, count, stride=PITCH), :].astype(jnp.bfloat16)
        split = lax.dot_general(place, values, (((1,), (1,)), ((), ())), preferred_element_type=jnp.float32)
        real, imag = split[:layers], split[layers:]
        m = pairs[:, :count] if h == 0 else (waves - 1.0) - pairs[:, :count]
        sin_half, cos_half = half_angle(m * shift, points, inverse)
        sines = 2.0 * sin_half * cos_half
        cosines = 1.0 - 2.0 * sin_half * sin_half
        for b in range(blocks):
            at = pl.ds(b * layers, layers)
            if b == 0:
                turned_real, turned_imag = real, imag
            else:
                cos_b, sin_b = cosines[b : b + 1], sines[b : b + 1]
                turned_real = real * cos_b - imag * sin_b
                turned_imag = real * sin_b + imag * cos_b
            turned[h, at, :count] = turned_real.astype(jnp.bfloat16)
            turned[2 + h, at, :count] = turned_imag.astype(jnp.bfloat16)


def multiply(turned, columns):
    lhs = jnp.concatenate([turned[k] for k in range(4)], axis=1)
    return jnp.dot(lhs, jnp.concatenate(columns, axis=1), preferred_element_type=jnp.float32)


def longitudes(latitude):
    return 20 + 4 * jnp.minimum(latitude, NLAT - 1 - latitude)


def exchange_kernel(
    waves,
    slots,
    fold,
    order,
    pair_hbm,
    pairs_hbm,
    lat_hbm,
    leg_hbm,
    spec_hbm,
    late_ref,
    table,
    sums,
    lanes,
    lengths,
    pair_ref,
    pairs_ref,
    lat_ref,
    leg_ref,
    spec_ref,
    held,
    rhs,
    ready,
    column,
    early,
    flat,
    turned,
    load_sem,
    send_sem,
    recv_sem,
    out_send,
    out_recv,
):
    wav_count = lax.axis_size("wav")
    lev_count = lax.axis_size("lev")
    w = lax.axis_index("wav")
    z = lax.axis_index("lev")
    right = lax.rem(z + 1, lev_count)
    left = lax.rem(z + lev_count - 1, lev_count)
    block = leg_ref.shape[1]
    full = (fold // 128) * 128
    rest = fold - full
    per_slot = full // 128
    chunks = held.shape[1]
    chunk = held.shape[2]
    rows = table.shape[1]
    total_slots = column.shape[0]

    sources = ((leg_hbm, leg_ref), (pair_hbm, pair_ref), (pairs_hbm, pairs_ref), (lat_hbm, lat_ref), (spec_hbm, spec_ref))
    loads = [pltpu.make_async_copy(src, dst, load_sem.at[i]) for i, (src, dst) in enumerate(sources)]
    for load in loads:
        load.start()

    barrier = pltpu.get_barrier_semaphore()
    for peer in (left, right):
        pl.semaphore_signal(barrier, inc=1, device_id={"lev": peer}, device_id_type=MESH)

    def greet(k, _):
        peer = lax.rem(w + k, wav_count)
        pl.semaphore_signal(barrier, inc=1, device_id={"wav": peer}, device_id_type=MESH)
        return 0

    lax.fori_loop(1, wav_count, greet, 0)

    loads[0].wait()
    tail = jnp.zeros((block, 128), jnp.float32)
    for s in range(slots):
        at_row = lax.broadcasted_iota(jnp.int32, (rest, 128), 0)
        at_col = lax.broadcasted_iota(jnp.int32, (rest, 128), 1)
        place = (at_col == at_row + rest * s).astype(jnp.bfloat16)
        tail += jnp.dot(leg_ref[s, :, full:fold], place, preferred_element_type=jnp.float32)
    held[z, 0, 0] = tail.astype(jnp.bfloat16)
    for s in range(slots):
        for k in range(per_slot):
            i = 1 + s * per_slot + k
            held[z, i // chunk, i % chunk] = leg_ref[s, :, k * 128 : (k + 1) * 128]

    pl.semaphore_wait(barrier, 2 + wav_count - 1)

    half = lev_count // 2

    def goes(side, d, c):
        return d < half - 1 or c % 2 == side

    def hop(side, d, c):
        owner = lax.rem(z + (lev_count - d if side == 0 else d), lev_count)
        return pltpu.make_async_remote_copy(
            src_ref=held.at[owner, c],
            dst_ref=held.at[owner, c],
            send_sem=send_sem.at[side, d, c],
            recv_sem=recv_sem.at[side, d, c],
            device_id={"lev": right if side == 0 else left},
            device_id_type=MESH,
        )

    def arrived(side, d, c):
        owner = lax.rem(z + (lev_count - d - 1 if side == 0 else d + 1), lev_count)
        pltpu.make_async_remote_copy(
            src_ref=held.at[owner, c],
            dst_ref=held.at[owner, c],
            send_sem=send_sem.at[side, d, c],
            recv_sem=recv_sem.at[side, d, c],
            device_id={"lev": right if side == 0 else left},
            device_id_type=MESH,
        ).wait_recv()

    def step(d, c):
        for side in (0, 1):
            if d:
                arrived(side, d - 1, c)
            if goes(side, d, c):
                hop(side, d, c).start()

    landed = set()

    def last(c):
        if c not in landed:
            landed.add(c)
            arrived(c % 2, half - 1, c)

    def mask_slot(s):
        border = (fold - 1) - pair_ref[w * slots + s]
        at_row = lax.broadcasted_iota(jnp.int32, (128, rest), 0)
        at_col = lax.broadcasted_iota(jnp.int32, (128, rest), 1)
        place = (at_row == at_col + rest * s).astype(jnp.bfloat16)
        row = lax.broadcasted_iota(jnp.int32, (128, 128), 0)
        ending = jnp.dot(place, spec_ref[s, full:fold, :], preferred_element_type=jnp.float32)
        below = row - rest * s + full < border
        rhs[s, 0:128, 0:128] = jnp.where(below, ending, 0.0).astype(jnp.bfloat16)
        rhs[s, 0:128, 128:256] = jnp.where(below, 0.0, ending).astype(jnp.bfloat16)
        for k in range(per_slot):
            piece = spec_ref[s, k * 128 : (k + 1) * 128, :].astype(jnp.float32)
            below = row + k * 128 < border
            at = (k + 1) * 128
            rhs[s, at : at + 128, 0:128] = jnp.where(below, piece, 0.0).astype(jnp.bfloat16)
            rhs[s, at : at + 128, 128:256] = jnp.where(below, 0.0, piece).astype(jnp.bfloat16)

    def start_basis():
        pairs = pairs_ref[...].astype(jnp.float32)
        for g in range(2):
            lined = lined_up(pairs, EARLY * g, slots if g else EARLY, wav_count, slots)
            lanes[:, g * 128 : (g + 1) * 128] = lined
            column[g * 128 : (g + 1) * 128, :] = jnp.transpose(jnp.broadcast_to(lined[:1], (128, 128)))

    strip = 32
    strips = total_slots // strip

    def basis_piece(i, _):
        r = lax.div(i, strips)
        block_of = lax.rem(i, strips)
        first = pl.multiple_of(block_of * strip, strip)
        group = lax.div(block_of, 4)
        local = pl.multiple_of(lax.rem(block_of, 4) * strip, strip)
        lon = longitudes(lat_ref[w * rows + r])
        highest = jnp.minimum(waves - 1, lax.shift_right_arithmetic(lon - 1, 1)).astype(jnp.float32)
        count = jnp.full((strip, 128), lon.astype(jnp.float32), jnp.float32)
        inverse = 1.0 / count
        lane = lax.broadcasted_iota(jnp.int32, (strip, 128), 1).astype(jnp.float32)
        pair = column[pl.ds(first, strip), :]
        for h in range(2):
            m = pair if h == 0 else (waves - 1.0) - pair
            weight = jnp.where(m == 0.0, 1.0, 2.0)
            weight = jnp.where((pair >= 0.0) & (m <= highest), weight, 0.0)
            minus = -2.0 * weight
            for c in range(WIDTH // 128):
                sin_half, cos_half = half_angle(m * (lane + 128.0 * c), count, inverse)
                scaled = sin_half * minus
                cos_part = (weight + scaled * sin_half).astype(jnp.bfloat16)
                sin_part = (scaled * cos_half).astype(jnp.bfloat16)
                table[group, r, c, pl.ds(h * 128 + local, strip), :] = cos_part
                table[group, r, c, pl.ds(256 + h * 128 + local, strip), :] = sin_part
        return 0

    made = [0]

    def more_basis(n):
        until = min(made[0] + n, rows * strips)
        if until > made[0]:
            lax.fori_loop(made[0], until, basis_piece, 0)
            made[0] = until

    def one_slot(s):
        parts = [0] + [1 + s * per_slot + k for k in range(per_slot)]
        for i in parts:
            last(i // chunk)
        total = None
        for a in range(0, len(parts), 2):
            pieces = [
                held[:, i // chunk, i % chunk].reshape(lev_count * block, 128) for i in parts[a : a + 2]
            ]
            lhs = jnp.concatenate(pieces, axis=1)
            term = jnp.dot(lhs, rhs[s, a * 128 : (a + 2) * 128], preferred_element_type=jnp.float32)
            total = term if total is None else total + term
        groups = total.reshape(wav_count, total.shape[0] // wav_count, 256)
        both = jnp.concatenate([groups[:, :, :128], groups[:, :, 128:]], axis=1)
        ready[s] = both.astype(jnp.bfloat16)

        place = early.at[s, w] if s < EARLY else late_ref.at[s - EARLY, w]

        def send(k, _):
            peer = lax.rem(w + k, wav_count)
            pltpu.make_async_remote_copy(
                src_ref=ready.at[s, peer],
                dst_ref=place,
                send_sem=out_send,
                recv_sem=out_recv.at[s],
                device_id={"wav": peer},
                device_id_type=MESH,
            ).start()
            return 0

        lax.fori_loop(1, wav_count, send, 0)
        if s < EARLY:
            early[s, w] = ready[s, w]
        else:
            late_ref[s - EARLY, w] = ready[s, w]

    for entry in order:
        kind, value = entry[0], entry[1:]
        if kind == "hop":
            step(*value)
        elif kind == "slot":
            one_slot(*value)
        elif kind == "basis":
            more_basis(*value)
        elif kind == "mask":
            loads[1].wait()
            loads[4].wait()
            for s in range(slots):
                mask_slot(s)
        else:
            loads[2].wait()
            loads[3].wait()
            start_basis()
    more_basis(rows * strips)
    for c in range(chunks):
        last(c)

    def arrival(s):
        target = early.at[s, 1:] if s < EARLY else late_ref.at[s - EARLY, 1:]
        pltpu.make_async_copy(target, target, out_recv.at[s]).wait()

    for s in range(EARLY):
        arrival(s)
    both = early.shape[2]
    for s in range(EARLY):
        unpack(flat.at[pl.ds(s * wav_count * PITCH, wav_count * PITCH)], early.at[s].reshape(wav_count * both, 128), wav_count, both)

    turned[...] = jnp.zeros_like(turned)

    def one_row(r, _):
        lengths[r] = jnp.full((8, 128), longitudes(lat_ref[w * rows + r]).astype(jnp.float32), jnp.float32)
        turn_row(waves, rows, 64, sums.shape[1] // 64, EARLY * wav_count, lanes[:, :128], flat, r, lengths[r][:, : EARLY * wav_count], turned)
        sums[r] = multiply(turned, [table[0, r, c] for c in range(WIDTH // 128)])
        return 0

    lax.fori_loop(0, rows, one_row, 0, unroll=2)

    for side in (0, 1):
        for d in range(half):
            for c in range(chunks):
                if goes(side, d, c):
                    hop(side, d, c).wait_send()

    pltpu.make_async_copy(ready.at[:, 1:], ready.at[:, 1:], out_send).wait()
    for s in range(EARLY, slots):
        arrival(s)


def plan(slots):
    hops = [(0, c) for c in (0, 1, 2, 3, 8, 5, 10, 4, 6, 9)]
    order = [("hop", *hop) for hop in hops]
    order += [("mask",), ("start",), ("basis", 24)]
    later = [(1, 0), (1, 1), (1, 2), (0, 7), (1, 3), (1, 5), (1, 8), (1, 4), (1, 6), (1, 9), (2, 0), (2, 1)]
    later += [(1, 10), (2, 2), (2, 3), (2, 5), (1, 7), (2, 4), (2, 6), (3, 0), (2, 8), (3, 1), (2, 10), (3, 2)]
    later += [(2, 9), (3, 4), (3, 3), (3, 8), (3, 6), (2, 7), (3, 5)]
    for i, hop in enumerate(later):
        order.append(("hop", *hop))
        if i % 3 == 2:
            order.append(("basis", 4))
    order += [("slot", 0), ("hop", 3, 10), ("slot", 1), ("hop", 3, 7), ("hop", 3, 9)]
    return order + [("slot", s) for s in range(2, slots)]


def exchange(spectral, legendre, wave_pair, lat_slot):
    slots, fold, _ = spectral.shape
    wav_count = lax.axis_size("wav")
    lev_count = lax.axis_size("lev")
    block = legendre.shape[2]
    rows = block * lev_count // wav_count
    total = wave_pair.shape[0]
    turned = jnp.swapaxes(legendre, 1, 2)
    tiles = 1 + slots * (fold // 128)
    chunk = 2
    chunks = tiles // chunk
    half = lev_count // 2
    moved = (2 * NLAT + 16 + WIDTH - 1) // WIDTH * 64
    return pl.pallas_call(
        functools.partial(exchange_kernel, fold - 1, slots, fold, plan(slots)),
        out_shape=[
            jax.ShapeDtypeStruct((slots - EARLY, wav_count, 2 * rows, 128), jnp.bfloat16),
            jax.ShapeDtypeStruct((2, rows, WIDTH // 128, 512, 128), jnp.bfloat16),
            jax.ShapeDtypeStruct((rows, moved, WIDTH), jnp.float32),
            jax.ShapeDtypeStruct((8, 256), jnp.float32),
            jax.ShapeDtypeStruct((rows, 8, 128), jnp.float32),
        ],
        in_specs=[pl.BlockSpec(memory_space=pl.ANY)] * 5,
        out_specs=[pl.BlockSpec(memory_space=pltpu.VMEM)] * 5,
        scratch_shapes=[
            pltpu.SMEM(wave_pair.shape, jnp.int32),
            pltpu.VMEM((1, total), jnp.int32),
            pltpu.SMEM(lat_slot.shape, jnp.int32),
            pltpu.VMEM(turned.shape, jnp.bfloat16),
            pltpu.VMEM(spectral.shape, jnp.bfloat16),
            pltpu.VMEM((lev_count, chunks, chunk, block, 128), jnp.bfloat16),
            pltpu.VMEM((slots, 512, 256), jnp.bfloat16),
            pltpu.VMEM((slots, wav_count, 2 * rows, 128), jnp.bfloat16),
            pltpu.VMEM((256, 128), jnp.float32),
            pltpu.VMEM((EARLY, wav_count, 2 * rows, 128), jnp.bfloat16),
            pltpu.VMEM((EARLY * wav_count * PITCH, 128), jnp.float32),
            pltpu.VMEM((4, moved, 128), jnp.bfloat16),
            pltpu.SemaphoreType.DMA((5,)),
            pltpu.SemaphoreType.DMA((2, half, chunks)),
            pltpu.SemaphoreType.DMA((2, half, chunks)),
            pltpu.SemaphoreType.DMA,
            pltpu.SemaphoreType.DMA((slots,)),
        ],
        compiler_params=pltpu.CompilerParams(
            collective_id=0, has_side_effects=True, vmem_limit_bytes=GRANT
        ),
        name="exchange",
    )(*(pltpu.with_memory_space_constraint(x, pltpu.HBM) for x in (wave_pair, wave_pair.reshape(1, total), lat_slot, turned, spectral)))


def synthesis_kernel(waves, together, in_ref, table, sums, lanes, lengths, out_ref, flat, *turned):
    step = pl.program_id(0)
    layers = out_ref.shape[1]
    width = out_ref.shape[2]
    blocks = (width + WIDTH - 1) // WIDTH
    count = flat.shape[0] // PITCH
    both = in_ref.shape[0] // count

    @pl.when(step == 0)
    def _():
        unpack(flat, in_ref, count, both)
        if count < 128:
            for buffer in turned:
                buffer[...] = jnp.zeros_like(buffer)

    for i in range(together):
        r = step * together + i
        turn_row(waves, both // 2, layers, blocks, count, lanes[:, 128:], flat, r, lengths[i][:, :count], turned[i])

    for i in range(together):
        result = sums[i] + multiply(turned[i], [table[0, i, c] for c in range(WIDTH // 128)])
        length = jnp.concatenate([lengths[i][:1]] * (WIDTH // 128), axis=1)
        for b in range(blocks):
            size = min(WIDTH, width - b * WIDTH)
            col = (lax.broadcasted_iota(jnp.int32, (layers, size), 1) + b * WIDTH).astype(jnp.float32)
            piece = result[b * layers : (b + 1) * layers, :size]
            piece = jnp.where(col < length[:, :size], piece, 0.0).astype(jnp.bfloat16)
            out_ref[i, :, b * WIDTH : b * WIDTH + size] = piece


def synthesis(late, table, sums, lanes, lengths, waves):
    held, wav_count, both, _ = late.shape
    rows = both // 2
    layers = 64
    width = 2 * NLAT + 16
    together = 4
    flat = late.reshape(held * wav_count * both, 128)
    return pl.pallas_call(
        functools.partial(synthesis_kernel, waves, together),
        grid=(rows // together,),
        out_shape=jax.ShapeDtypeStruct((rows, layers, width), jnp.bfloat16),
        in_specs=[
            pl.BlockSpec(flat.shape, lambda r: (0, 0)),
            pl.BlockSpec((1, together, *table.shape[2:]), lambda r: (1, r, 0, 0, 0)),
            pl.BlockSpec((together, *sums.shape[1:]), lambda r: (r, 0, 0)),
            pl.BlockSpec(lanes.shape, lambda r: (0, 0)),
            pl.BlockSpec((together, *lengths.shape[1:]), lambda r: (r, 0, 0)),
        ],
        out_specs=pl.BlockSpec((together, layers, width), lambda r: (r, 0, 0)),
        scratch_shapes=[
            pltpu.VMEM((held * wav_count * PITCH, 128), jnp.float32),
        ]
        + [pltpu.VMEM((4, sums.shape[1], 128), jnp.bfloat16)] * together,
        compiler_params=pltpu.CompilerParams(
            dimension_semantics=("arbitrary",), vmem_limit_bytes=GRANT
        ),
        name="synthesis",
    )(flat, table, sums, lanes, lengths)


def on_device(spectral, legendre, wave_pair, lat_slot):
    late, table, sums, lanes, lengths = exchange(spectral, legendre, wave_pair, lat_slot)
    return synthesis(late, table, sums, lanes, lengths, spectral.shape[1] - 1)


def solution(mesh):
    return jax.shard_map(
        on_device,
        mesh=mesh,
        in_specs=(P("wav", None, "lev"), P("wav", None, "lev"), P(), P()),
        out_specs=P("wav", "lev", None),
        check_vma=False,
    )
```
